32 devices in a mesh: ga: 2 (over x), row: 8 (over z, y), col: 2 (over core).
Axes of the slice: x: 2, y: 2, z: 4, core: 2. Of those that a mesh axis runs over, the one named last changes fastest.
Arguments:
- pair: bfloat16 [256, 128, 128], P(('ga', 'row', 'col')), parts along dimension 0, may hold values from -480 to 480
- residue_mask: int32 [256], P('ga'), parts along dimension 0, may hold values from 0 to 1, as said below
- targets: int32 [256, 128], P(('ga', 'row', 'col')), parts along dimension 0, may hold values from 0 to 63
- ln_gain: float32 [2, 128], replicated, may hold values from 0.25 to 1.75
- ln_shift: float32 [2, 128], replicated, may hold values from -3 to 3
- w_in: bfloat16 [5, 128, 128], P(None, None, 'col'), may hold values from -0.5 to 0.5
- b_in: float32 [5, 128], replicated, may hold values from -3 to 3
- w_out: bfloat16 [128, 128], P('col'), may hold values from -0.5 to 0.5
- b_out: float32 [128], replicated, may hold values from -3 to 3
- head_weight: bfloat16 [128, 64], replicated, may hold values from -0.5 to 0.5
- head_bias: float32 [64], replicated, may hold values from -4 to 4
Outputs:
- update: bfloat16 [256, 128, 128], P(('ga', 'row', 'col')), parts along dimension 0
- pair_loss: float32 [256, 128], P(('ga', 'row', 'col')), parts along dimension 0
The draws below stay inside these ranges and needn't reach their ends.
There are 2 independent parts, one for each index of `ga`. The reference program is written for one: setup_inputs(seed, part) draws one part's arguments, and reference() takes and returns one part's arrays. A program takes and returns all parts, laid end to end along the dimension named above; an argument that names none is the same for every part. Nothing has to cross between parts.
Inputs may be any that keep to these rules, and one draw needn't show every extreme that they name: `residue_mask`: each part's entries are 1 for residues 0 to some length - 1 and 0 after it; the length is at least 64 and at most 128.
All inputs are finite; a program needn't handle non-finite values.
Results may differ from the reference program's by a relative error of at most 0.0055.
Values may be sent and summed in bfloat16 or wider, within the bound.
A program may use at most 64 MiB of HBM per device.

```python
import jax
import jax.numpy as jnp
from jax import lax

D = 128
BINS = 64
RESIDUES = 128


def draw_pair(key, part):
    first_key, second_key = jax.random.split(key)
    values = jnp.clip(jax.random.normal(first_key, (RESIDUES, RESIDUES, D), jnp.float32), -6.0, 6.0)
    return values.astype(jnp.bfloat16)


def draw_residue_mask(key, part):
    crop_length = jax.random.randint(key, (), RESIDUES // 2, RESIDUES + 1)
    return (jnp.arange(RESIDUES) < crop_length).astype(jnp.int32)


def set_ends(result, key, smallest, largest):
    extent = result.shape
    spot = [jax.random.randint(jax.random.fold_in(key, axis), (), 0, extent[axis]) for axis in range(len(extent))]
    result = result.at[tuple(spot)].set(smallest)
    longest = extent.index(max(extent))
    spot[longest] = (spot[longest] + 1) % extent[longest]
    return result.at[tuple(spot)].set(largest)


def shard_levels(key, dims, pieces, least, high):
    gain, own = 1.0, jax.random.fold_in(key, 6)
    for dim, parts in pieces:
        steps = jnp.exp(jax.random.uniform(jax.random.fold_in(own, dim), (parts,), jnp.float32, least / len(pieces), high / len(pieces)))
        gain = gain * jnp.repeat(steps, dims[dim] // parts).reshape([-1 if axis == dim else 1 for axis in range(len(dims))])
    return gain


def gaussian(own_key, dims, scale, bound, cuts=(), kind=jnp.bfloat16):
    drawn = scale * jax.random.normal(own_key, dims, jnp.float32)
    if cuts:
        drawn = drawn * shard_levels(own_key, dims, cuts, -0.22, 0.18)
    return jnp.clip(drawn, -bound, bound).astype(kind)


def setup_inputs(seed: int = 0, part: int = 0) -> dict:
    key_list = jax.random.split(jax.random.key(seed), 12)
    part_keys = jax.random.split(jax.random.fold_in(key_list[11], part), 12)
    pair = draw_pair(jax.random.fold_in(jax.random.fold_in(key_list[11], part), 71), part)
    residue_mask = draw_residue_mask(jax.random.fold_in(jax.random.fold_in(key_list[11], part), 71), part)
    targets = set_ends(jax.random.randint(part_keys[2], (RESIDUES, RESIDUES), 0, BINS), jax.random.fold_in(part_keys[2], 1), 0, BINS - 1).astype(jnp.int32)
    ln_gain = jnp.clip(1.0 + 0.15 * jax.random.normal(key_list[3], (2, D), jnp.float32), 0.25, 1.75)
    ln_shift = gaussian(key_list[4], (2, D), 0.3, 3.0, (), jnp.float32)
    w_in = gaussian(key_list[5], (5, D, D), D ** -0.5, 0.5, ((2, 2),))
    b_in = gaussian(key_list[6], (5, D), 0.5, 3.0, (), jnp.float32)
    w_out = gaussian(key_list[7], (D, D), D ** -0.5, 0.5, ((0, 2),))
    b_out = gaussian(key_list[8], (D,), 0.5, 3.0, (), jnp.float32)
    head_weight = gaussian(key_list[9], (D, BINS), D ** -0.5, 0.5)
    head_bias = gaussian(key_list[10], (BINS,), 1.0, 4.0, (), jnp.float32)
    return dict(pair=pair, residue_mask=residue_mask, targets=targets, ln_gain=ln_gain, ln_shift=ln_shift, w_in=w_in, b_in=b_in, w_out=w_out, b_out=b_out, head_weight=head_weight, head_bias=head_bias)


def normalize(values, gain_vec, shift_vec, epsilon):
    average = lax.optimization_barrier(jnp.mean(values, axis=-1, keepdims=True))
    centred = values - average
    spread = lax.optimization_barrier(jnp.mean(centred * centred, axis=-1, keepdims=True))
    return centred * lax.rsqrt(spread + epsilon) * gain_vec + shift_vec

def reference(pair, residue_mask, targets, ln_gain, ln_shift, w_in, b_in, w_out, b_out, head_weight, head_bias):
    res_mask = residue_mask.astype(jnp.float32)
    row_block = 32
    block_count = RESIDUES // row_block
    pair_blocks = pair.reshape(block_count, row_block, RESIDUES, D)
    mask_blocks = res_mask.reshape(block_count, row_block)
    weights_in = w_in.astype(jnp.float32)

    def project(operands):
        rows_pair, rows_mask = operands
        normed = normalize(rows_pair.astype(jnp.float32), ln_gain[0], ln_shift[0], 0.1).astype(jnp.bfloat16)
        projected = jnp.einsum('ikc,ncd->nikd', normed.astype(jnp.float32), weights_in) + b_in[:, None, None, :]
        masks = rows_mask[:, None, None] * res_mask[None, :, None]
        left_side = (masks * jax.nn.sigmoid(projected[1]) * projected[0]).astype(jnp.bfloat16)
        right_side = (masks * jax.nn.sigmoid(projected[3]) * projected[2]).astype(jnp.bfloat16)
        gate_value = jax.nn.sigmoid(projected[4])
        return (left_side, right_side, gate_value)
    lefts, rights, gates = lax.map(project, (pair_blocks, mask_blocks))
    left_chan = jnp.transpose(lefts.reshape(RESIDUES, RESIDUES, D), (2, 0, 1))
    right_chan = jnp.transpose(rights.reshape(RESIDUES, RESIDUES, D), (2, 0, 1))

    def triangle(operands):
        left_part, right_part = operands
        product = jnp.einsum('cik,cjk->cij', left_part.astype(jnp.float32), right_part.astype(jnp.float32))
        return product.astype(jnp.bfloat16)
    outer_prod = lax.map(triangle, (left_chan.reshape(D // 8, 8, RESIDUES, RESIDUES), right_chan.reshape(D // 8, 8, RESIDUES, RESIDUES)))
    outer_rows = jnp.transpose(outer_prod.reshape(D, RESIDUES, RESIDUES), (1, 2, 0))
    weights_out = w_out.astype(jnp.float32)
    head_float = head_weight.astype(jnp.float32)

    def finish(operands):
        rows_outer, rows_gate, rows_pair = operands
        normed_outer = normalize(rows_outer.astype(jnp.float32), ln_gain[1], ln_shift[1], 1.0).astype(jnp.bfloat16)
        mixed = jnp.einsum('ijc,cd->ijd', normed_outer.astype(jnp.float32), weights_out) + b_out
        update = (rows_gate * mixed).astype(jnp.bfloat16)
        new_pair = (rows_pair.astype(jnp.float32) + update.astype(jnp.float32)).astype(jnp.bfloat16)
        logits = jnp.einsum('ijc,cb->ijb', new_pair.astype(jnp.float32), head_float) + head_bias
        return (update, logits)
    updates, logit_blocks = lax.map(finish, (outer_rows.reshape(block_count, row_block, RESIDUES, D), gates, pair_blocks))
    update = updates.reshape(RESIDUES, RESIDUES, D)
    logits = logit_blocks.reshape(RESIDUES, RESIDUES, BINS)
    symmetric = logits + jnp.transpose(logits, (1, 0, 2))
    log_total = jax.nn.logsumexp(symmetric, axis=-1)
    picked = jnp.take_along_axis(symmetric, targets[..., None].astype(jnp.int32), axis=-1)[..., 0]
    pair_loss = res_mask[:, None] * res_mask[None, :] * (log_total - picked)
    return (update, pair_loss)
```

```python
import functools

import jax
import jax.numpy as jnp
from jax import lax
from jax.experimental import pallas as pl
from jax.experimental.pallas import tpu as pltpu
from jax.sharding import PartitionSpec as P

SUPER = 2
F32, BF16 = jnp.float32, jnp.bfloat16
NT = (((1,), (1,)), ((), ()))
TN = (((0,), (0,)), ((), ()))


def dot(lhs, rhs, dims=(((1,), (0,)), ((), ()))):
    return lax.dot_general(lhs, rhs, dims, preferred_element_type=F32)


def kernel(
    rows_n, cols_n, sup,
    *refs,
):
    sources, (update, loss) = refs[:11], refs[11:13]
    held, rest = refs[13:24], refs[24:]
    (pair, mask, targets, ln_gain, ln_shift, w_in, b_in, w_out, b_out, head_w, head_b) = held
    (
    wt, wo, small, normed, side_f, right_b, left_b, left_in, right_in, prod, outer, outer_f, gate,
        new_pair, logit_b, logit_in, logit_f, own_t,
        w_send, w_recv, l_send, l_recv, r_send, r_recv, o_send, o_recv, m_send, m_recv,
        in_sem,
    ) = rest
    groups = rows_n * cols_n
    count, length, width = pair.shape
    bins = head_w.shape[0]
    per = groups // sup
    share = width // per
    part = share // cols_n
    half = w_in.shape[1]
    lanes = 128
    spans = length // lanes
    packed = 128 // bins
    quads = count // packed
    col = lax.axis_index("col")
    me = lax.axis_index("row") * cols_n + col
    block, slot = lax.div(me, per), lax.rem(me, per)
    plane = per // 2
    inner = (lax.div(slot, plane) + block) % 2 == 1

    def where(peer):
        return {"row": lax.div(peer, cols_n), "col": lax.rem(peer, cols_n)}

    def remote(src, dst, send, recv, peer):
        return pltpu.make_async_remote_copy(
            src_ref=src, dst_ref=dst, send_sem=send, recv_sem=recv,
            device_id=where(peer), device_id_type=pl.DeviceIdType.MESH,
        )

    def each(n, body):
        lax.fori_loop(0, n, lambda i, c: (body(i), c)[1], 0, unroll=True)

    loads = [pltpu.make_async_copy(sources[n], held[n], in_sem.at[n]) for n in range(11)]
    for load in loads:
        load.start()
    barrier = pltpu.get_barrier_semaphore()

    def greet(d):
        pl.semaphore_signal(
            barrier, inc=1, device_id=where(lax.rem(me + 1 + d, groups)),
            device_id_type=pl.DeviceIdType.MESH,
        )

    each(groups - 1, greet)

    def drain(ref, sem):
        pltpu.make_async_copy(ref, ref, sem).wait()


    for load in loads:
        load.wait()
    mine = pl.ds(pl.multiple_of(col * half, half), half)
    wt[:, mine, :] = w_in[...]
    wo[mine, :] = w_out[...]

    def norm_rows(i):
        values = pair[i].astype(F32)
        centred = values - jnp.mean(values, axis=-1, keepdims=True)
        spread = jnp.mean(centred * centred, axis=-1, keepdims=True)
        scaled = centred * lax.rsqrt(spread + 0.1) * ln_gain[0:1, :] + ln_shift[0:1, :]
        normed[i] = scaled.astype(BF16)

    each(count, norm_rows)

    row_mask = mask[...].astype(F32)
    lane = lax.broadcasted_iota(jnp.int32, (count, length), 1)
    sub = lax.broadcasted_iota(jnp.int32, (count, length), 0)
    own_mask = jnp.sum(jnp.where(lane == me * count + sub, row_mask, 0.0), axis=1, keepdims=True)
    pair_mask = own_mask * row_mask

    small[...] = jnp.concatenate(
        [b_in[...], ln_gain[1:2, :], ln_shift[1:2, :], jnp.zeros((1, width), F32)], axis=0
    ).T

    def weight_copies(peer_col):
        peer = me - col + peer_col
        return (
            remote(wt.at[:, mine, :], wt.at[:, mine, :], w_send.at[0, peer_col], w_recv.at[0, col], peer),
            remote(wo.at[mine, :], wo.at[mine, :], w_send.at[1, peer_col], w_recv.at[1, col], peer),
        )

    def wait_weights(which):
        for d in range(1, cols_n):
            peer_col = lax.rem(col + d, cols_n)
            theirs = pl.ds(pl.multiple_of(peer_col * half, half), half)
            ref = (wt.at[:, theirs, :], wo.at[theirs, :])[which]
            mine_ref = (wt.at[:, mine, :], wo.at[mine, :])[which]
            peer = me - col + peer_col
            remote(ref, ref, w_send.at[which, peer_col], w_recv.at[which, peer_col], peer).wait_recv()
            remote(mine_ref, mine_ref, w_send.at[which, peer_col], w_recv.at[which, peer_col], peer).wait_send()

    def make_side(first, out, span_w):
        start = pl.multiple_of(span_w * half, half)
        rows = pl.ds(start, half)
        weights = wt[first:first + 2, rows, :].reshape(2 * half, width)
        value_b, gate_b = small[rows, first:first + 1], small[rows, first + 1:first + 2]

        for i in range(count):
            both = dot(weights, normed[i], NT)
            value = jax.nn.sigmoid(both[half:] + gate_b) * (both[:half] + value_b)
            for b in range(spans):
                side_f[b, pl.ds(i, half, stride=count), :] = value[:, b * lanes:(b + 1) * lanes]
        for b in range(spans):
            span = slice(b * lanes, (b + 1) * lanes)
            masked = side_f[b].reshape(half, count, lanes) * pair_mask[:, span][None]
            out[rows, :, span] = masked.astype(BF16)

    def channels(owner, h):
        return pl.ds(h * half + owner * part, part)

    def places(h):
        return pl.ds(h * part, part)

    def left_copy(dest, h):
        return remote(
            left_b.at[channels(dest, h)], left_in.at[slot, places(h)],
            l_send.at[h], l_recv.at[h], block * per + dest,
        )

    def right_copy(dest, h):
        return remote(
            right_b.at[channels(lax.rem(dest, per), h)], right_in.at[me, places(h)],
            r_send.at[h], r_recv.at[h], dest,
        )

    def send_block(h):
        def one(d):
            owner = lax.rem(slot + 1 + d, per)
            right_copy(block * per + owner, h).start()
            left_copy(owner, h).start()

        each(per - 1, one)

    def send_across(h):
        def one(d):
            near = lax.rem(lax.div(d, plane) + block, 2)
            owner = near * plane + lax.rem(slot + d, plane)
            right_copy((1 - block) * per + owner, h).start()

        each(per, one)

    def keep(h):
        pltpu.make_async_copy(right_b.at[channels(slot, h)], right_in.at[me, places(h)], r_recv.at[h]).start()
        pltpu.make_async_copy(left_b.at[channels(slot, h)], left_in.at[slot, places(h)], l_recv.at[h]).start()

    make_side(2, right_b, col)
    pl.semaphore_wait(barrier, groups - 1)
    for d in range(1, cols_n):
        for copy in weight_copies(lax.rem(col + d, cols_n)):
            copy.start()
    for turn in range(cols_n):
        h = lax.rem(col + turn, cols_n)
        if turn:
            if turn == 1:
                wait_weights(0)
            make_side(2, right_b, h)
        send_across(h)
        make_side(0, left_b, h)
        send_block(h)
        keep(h)


    def make_gate(i):
        gate[i] = jax.nn.sigmoid(dot(normed[i], wt[4], NT) + b_in[4:5, :])

    each(count, make_gate)
    wait_weights(1)

    def outer_copy(dest, h):
        return remote(
            prod.at[dest, places(h)], outer.at[channels(slot, h)],
            o_send.at[h], o_recv.at[h], block * per + dest,
        )

    for h in range(cols_n):
        drain(left_in.at[:, places(h)], l_recv.at[h])
        drain(right_in.at[:, places(h)], r_recv.at[h])
        for c in range(h * part, (h + 1) * part):
            lhs = left_in[:, c].reshape(per * count, length)
            rhs = right_in[:, c].reshape(length, length)
            prod[:, c] = dot(lhs, rhs, NT).astype(BF16).reshape(per, count, length)
        each(per - 1, lambda d: outer_copy(lax.rem(slot + 1 + d, per), h).start())
        pltpu.make_async_copy(prod.at[slot, places(h)], outer.at[channels(slot, h)], o_recv.at[h]).start()

    for h in range(cols_n):
        drain(prod.at[:, places(h)], o_recv.at[h])

    head_t = head_w[...]
    blank = jnp.zeros((bins, width), BF16)
    spread_w = [
        jnp.concatenate([head_t if h == p else blank for h in range(packed)], axis=0)
        for p in range(packed)
    ]
    bias_row = jnp.concatenate([head_b[...]] * packed, axis=1)

    gain_col, shift_col = small[:, 5:6], small[:, 6:7]
    for b in range(spans):
        span = slice(b * lanes, (b + 1) * lanes)
        values = outer[:, :, span].astype(F32)
        average = jnp.sum(values, axis=0) * (1.0 / width)
        outer_f[b] = values.reshape(width * count, lanes)
        centred = values - average[None]
        inverse = lax.rsqrt(jnp.sum(centred * centred, axis=0) * (1.0 / width) + 1.0)
        for i in range(count):
            part_i = outer_f[b, pl.ds(i, width, stride=count), :]
            part_i = (part_i - average[i:i + 1, :]) * inverse[i:i + 1, :] * gain_col + shift_col
            mixed = dot(part_i.astype(BF16), wo[...], TN) + b_out[...]
            rounded = (gate[i, span, :] * mixed).astype(BF16)
            update[i, span, :] = rounded
            new_pair[i, span, :] = (pair[i, span, :].astype(F32) + rounded.astype(F32)).astype(BF16)
    for i in range(quads):
        total = bias_row
        for p in range(packed):
            total = total + dot(new_pair[p * quads + i], spread_w[p], NT)
        logit_b[:, i] = total.astype(BF16).reshape(groups, count, 128)

    def logit_copy(dest):
        return remote(
            logit_b.at[dest], logit_in.at[me],
            m_send.at[0], m_recv.at[0], dest,
        )

    logit_local = pltpu.make_async_copy(
        logit_b.at[me], logit_in.at[me], m_recv.at[0]
    )
    each(groups - 1, lambda d: logit_copy(lax.rem(me + 1 + d, groups)).start())
    logit_local.start()

    bias_col = jnp.concatenate([head_b[...], jnp.zeros((7, bins), F32)], axis=0).T[:, 0:1]
    for i in range(count):
        own_t[i] = dot(head_t, new_pair[i], NT) + bias_col
    at = lax.broadcasted_iota(jnp.int32, (length, length), 0)
    to = lax.broadcasted_iota(jnp.int32, (length, length), 1)
    fold = length // packed
    order = ((at % fold) // quads) * count + (at // fold) * quads + at % quads
    shuffle = jnp.where(order == to, 1.0, 0.0).astype(BF16)

    drain(logit_in, m_recv.at[0])
    logit_f[...] = logit_in[...].astype(F32).reshape(logit_f.shape)
    bin_id = lax.broadcasted_iota(jnp.int32, (bins, length), 0)
    for i in range(count):
        flipped = logit_f[pl.ds(i, groups * quads, stride=count), :].T
        flipped = jnp.concatenate([flipped[p * bins:(p + 1) * bins] for p in range(packed)], axis=1)
        symmetric = own_t[i] + dot(flipped.astype(BF16), shuffle)
        top = jnp.max(symmetric, axis=0, keepdims=True)
        total = top + jnp.log(jnp.sum(jnp.exp(symmetric - top), axis=0, keepdims=True))
        chosen = jnp.sum(jnp.where(bin_id == targets[i:i + 1, :], symmetric, 0.0), axis=0, keepdims=True)
        loss[i:i + 1, :] = pair_mask[i:i + 1, :] * (total - chosen)

    for h in range(cols_n):
        drain(left_in.at[pl.ds(0, per - 1), places(h)], l_send.at[h])
        drain(right_in.at[pl.ds(0, groups - 1), places(h)], r_send.at[h])
        drain(prod.at[pl.ds(0, per - 1), places(h)], o_send.at[h])
    drain(logit_in.at[pl.ds(0, groups - 1)], m_send.at[0])


def finish(update, loss, update_out, loss_out, sem):
    first = pltpu.make_async_copy(update, update_out, sem.at[0])
    second = pltpu.make_async_copy(loss, loss_out, sem.at[1])
    first.start()
    second.start()
    first.wait()
    second.wait()


def local(rows_n, cols_n, *args):
    pair, residue_mask, targets, ln_gain, ln_shift, w_in, b_in, w_out, b_out, head_w, head_b = args
    count, length, width = pair.shape
    bins = head_w.shape[1]
    groups = rows_n * cols_n
    sup = SUPER
    per = groups // sup
    share = width // per
    chunks = cols_n
    packed = 128 // bins
    quads = count // packed
    dma = pltpu.SemaphoreType.DMA
    vmem = pl.BlockSpec(memory_space=pltpu.VMEM)
    inputs = (
        pair, residue_mask.reshape(1, length), targets, ln_gain, ln_shift,
        jnp.swapaxes(w_in, 1, 2), b_in, w_out, b_out.reshape(1, width), head_w.T,
        head_b.reshape(1, bins),
    )
    update, loss = pl.pallas_call(
        functools.partial(kernel, rows_n, cols_n, sup),
        out_shape=(
            pltpu.VMEM(pair.shape, BF16),
            pltpu.VMEM((count, length), F32),
        ),
        in_specs=[pl.BlockSpec(memory_space=pl.ANY)] * 11,
        out_specs=(vmem, vmem),
        scratch_shapes=[pltpu.VMEM(x.shape, x.dtype) for x in inputs] + [
            pltpu.VMEM((5, width, width), BF16),
            pltpu.VMEM((width, width), BF16),
            pltpu.VMEM((width, 8), F32),
            pltpu.VMEM((count, length, width), BF16),
            pltpu.VMEM((length // 128, width // cols_n * count, 128), F32),
            pltpu.VMEM((width, count, length), BF16),
            pltpu.VMEM((width, count, length), BF16),
            pltpu.VMEM((per, share, count, length), BF16),
            pltpu.VMEM((groups, share, count, length), BF16),
            pltpu.VMEM((per, share, count, length), BF16),
            pltpu.VMEM((width, count, length), BF16),
            pltpu.VMEM((length // 128, width * count, 128), F32),
            pltpu.VMEM((count, length, width), F32),
            pltpu.VMEM((count, length, width), BF16),
            pltpu.VMEM((groups, quads, count, 128), BF16),
            pltpu.VMEM((groups, quads, count, 128), BF16),
            pltpu.VMEM((groups * quads * count, 128), F32),
            pltpu.VMEM((count, bins, length), F32),
            dma((2, cols_n)), dma((2, cols_n)),
            dma((chunks,)), dma((chunks,)), dma((chunks,)), dma((chunks,)), dma((chunks,)), dma((chunks,)),
            dma((1,)), dma((1,)),
            dma((11,)),
        ],
        compiler_params=pltpu.CompilerParams(
            collective_id=0, has_side_effects=True, vmem_limit_bytes=60 * 1024 * 1024
        ),
    )(*inputs)
    anywhere = pl.BlockSpec(memory_space=pl.ANY)
    return pl.pallas_call(
        finish,
        out_shape=(
            jax.ShapeDtypeStruct(update.shape, update.dtype), jax.ShapeDtypeStruct(loss.shape, loss.dtype),
        ),
        in_specs=[pl.BlockSpec(memory_space=pltpu.VMEM)] * 2, compiler_params=pltpu.CompilerParams(vmem_limit_bytes=1024*1024),
        out_specs=(anywhere, anywhere),
        scratch_shapes=[dma((2,))],
    )(update, loss)


def solution(mesh):
    placed = (
        P(("ga", "row", "col"), None, None),
        P("ga"),
        P(("ga", "row", "col"), None),
        P(),
        P(),
        P(None, None, "col"),
        P(),
        P("col", None),
        P(),
        P(),
        P(),
    )
    return jax.shard_map(
        functools.partial(local, mesh.shape["row"], mesh.shape["col"]),
        mesh=mesh,
        in_specs=placed,
        out_specs=(P(("ga", "row", "col"), None, None), P(("ga", "row", "col"), None)),
        check_vma=False,
    )
```

```python
import functools

import jax
import jax.numpy as jnp
from jax import lax
from jax.experimental import pallas as pl
from jax.experimental.pallas import tpu as pltpu
from jax.sharding import PartitionSpec as P

SUPER = 2
CUT = 5
F32, BF16 = jnp.float32, jnp.bfloat16
NT = (((1,), (1,)), ((), ()))
TN = (((0,), (0,)), ((), ()))


def dot(lhs, rhs, dims=(((1,), (0,)), ((), ()))):
    return lax.dot_general(lhs, rhs, dims, preferred_element_type=F32)


def kernel(
    rows_n, cols_n, sup, chunks,
    *refs,
):
    sources, (update, loss) = refs[:11], refs[11:13]
    held, rest = refs[13:24], refs[24:]
    (pair, mask, targets, ln_gain, ln_shift, w_in, b_in, w_out, b_out, head_w, head_b) = held
    (
    wt, wo, small, normed, side_f, right_b, left_b, left_in, right_in, prod, outer, outer_f, gate,
        new_pair, logit_b, logit_in, logit_f, own_t,
        w_send, w_recv, l_send, l_recv, r_send, r_recv, o_send, o_recv, m_send, m_recv,
        in_sem,
    ) = rest
    groups = rows_n * cols_n
    count, length, width = pair.shape
    bins = head_w.shape[0]
    per = groups // sup
    share = width // per
    part = share // cols_n
    cut = max(part * CUT // 8, 1)
    edges = [0, cut, part]
    half = w_in.shape[1]
    lanes = 128
    spans = length // lanes
    packed = 128 // bins
    quads = count // packed
    col = lax.axis_index("col")
    me = lax.axis_index("row") * cols_n + col
    block, slot = lax.div(me, per), lax.rem(me, per)
    plane = per // 2

    def where(peer):
        return {"row": lax.div(peer, cols_n), "col": lax.rem(peer, cols_n)}

    def remote(src, dst, send, recv, peer):
        return pltpu.make_async_remote_copy(
            src_ref=src, dst_ref=dst, send_sem=send, recv_sem=recv,
            device_id=where(peer), device_id_type=pl.DeviceIdType.MESH,
        )

    def each(n, body):
        lax.fori_loop(0, n, lambda i, c: (body(i), c)[1], 0, unroll=True)

    loads = [pltpu.make_async_copy(sources[n], held[n], in_sem.at[n]) for n in range(11)]
    for load in loads:
        load.start()
    barrier = pltpu.get_barrier_semaphore()

    def greet(d):
        pl.semaphore_signal(
            barrier, inc=1, device_id=where(lax.rem(me + 1 + d, groups)),
            device_id_type=pl.DeviceIdType.MESH,
        )

    each(groups - 1, greet)

    def drain(ref, sem):
        pltpu.make_async_copy(ref, ref, sem).wait()


    for load in loads:
        load.wait()
    mine = pl.ds(pl.multiple_of(col * half, half), half)
    wt[:, mine, :] = w_in[...]
    wo[mine, :] = w_out[...]

    def norm_rows(i):
        values = pair[i].astype(F32)
        centred = values - jnp.mean(values, axis=-1, keepdims=True)
        spread = jnp.mean(centred * centred, axis=-1, keepdims=True)
        scaled = centred * lax.rsqrt(spread + 0.1) * ln_gain[0:1, :] + ln_shift[0:1, :]
        normed[i] = scaled.astype(BF16)

    each(count, norm_rows)

    row_mask = mask[...].astype(F32)
    lane = lax.broadcasted_iota(jnp.int32, (count, length), 1)
    sub = lax.broadcasted_iota(jnp.int32, (count, length), 0)
    own_mask = jnp.sum(jnp.where(lane == me * count + sub, row_mask, 0.0), axis=1, keepdims=True)
    pair_mask = own_mask * row_mask

    small[...] = jnp.concatenate(
        [b_in[...], ln_gain[1:2, :], ln_shift[1:2, :], jnp.zeros((1, width), F32)], axis=0
    ).T

    def weight_copies(peer_col):
        peer = me - col + peer_col
        return (
            remote(wt.at[:, mine, :], wt.at[:, mine, :], w_send.at[0, peer_col], w_recv.at[0, col], peer),
            remote(wo.at[mine, :], wo.at[mine, :], w_send.at[1, peer_col], w_recv.at[1, col], peer),
        )

    def wait_weights(which):
        for d in range(1, cols_n):
            peer_col = lax.rem(col + d, cols_n)
            theirs = pl.ds(pl.multiple_of(peer_col * half, half), half)
            ref = (wt.at[:, theirs, :], wo.at[theirs, :])[which]
            mine_ref = (wt.at[:, mine, :], wo.at[mine, :])[which]
            peer = me - col + peer_col
            remote(ref, ref, w_send.at[which, peer_col], w_recv.at[which, peer_col], peer).wait_recv()
            remote(mine_ref, mine_ref, w_send.at[which, peer_col], w_recv.at[which, peer_col], peer).wait_send()

    def make_side(first, out, span_w):
        start = pl.multiple_of(span_w * half, half)
        rows = pl.ds(start, half)
        weights = wt[first:first + 2, rows, :].reshape(2 * half, width)
        value_b, gate_b = small[rows, first:first + 1], small[rows, first + 1:first + 2]

        for i in range(count):
            both = dot(weights, normed[i], NT)
            value = jax.nn.sigmoid(both[half:] + gate_b) * (both[:half] + value_b)
            for b in range(spans):
                side_f[b, pl.ds(i, half, stride=count), :] = value[:, b * lanes:(b + 1) * lanes]
        for b in range(spans):
            span = slice(b * lanes, (b + 1) * lanes)
            masked = side_f[b].reshape(half, count, lanes) * pair_mask[:, span][None]
            out[span_w, :, :, span] = masked.astype(BF16)

    def channels(owner, ch):
        return pl.ds(owner * part + edges[ch], edges[ch + 1] - edges[ch])

    def places(ch):
        return pl.ds(edges[ch], edges[ch + 1] - edges[ch])

    def left_copy(dest, ch, h):
        return remote(
            left_b.at[h, channels(dest, ch)], left_in.at[slot, h, places(ch)],
            l_send.at[ch], l_recv.at[ch], block * per + dest,
        )

    def right_copy(dest, ch, h):
        return remote(
            right_b.at[h, channels(lax.rem(dest, per), ch)], right_in.at[me, h, places(ch)],
            r_send.at[ch], r_recv.at[ch], dest,
        )

    def send_block(ch, h):
        def one(d):
            owner = lax.rem(slot + 1 + d, per)
            right_copy(block * per + owner, ch, h).start()
            left_copy(owner, ch, h).start()

        each(per - 1, one)

    def send_across(ch, h):
        def one(d):
            near = lax.rem(lax.div(d, plane) + block, 2)
            owner = near * plane + lax.rem(slot + d, plane)
            right_copy((1 - block) * per + owner, ch, h).start()

        each(per, one)

    def keep(ch):
        pltpu.make_async_copy(
            right_b.at[:, channels(slot, ch)], right_in.at[me, :, places(ch)], r_recv.at[ch]
        ).start()
        pltpu.make_async_copy(
            left_b.at[:, channels(slot, ch)], left_in.at[slot, :, places(ch)], l_recv.at[ch]
        ).start()

    make_side(2, right_b, col)
    pl.semaphore_wait(barrier, groups - 1)
    for d in range(1, cols_n):
        for copy in weight_copies(lax.rem(col + d, cols_n)):
            copy.start()
    for turn in range(cols_n):
        h = lax.rem(col + turn, cols_n)
        if turn:
            if turn == 1:
                wait_weights(0)
            make_side(2, right_b, h)
        send_across(0, h)
        make_side(0, left_b, h)
        send_block(0, h)
    keep(0)
    every = slice(None)
    send_across(1, every)
    send_block(1, every)
    keep(1)


    def make_gate(i):
        gate[i] = jax.nn.sigmoid(dot(normed[i], wt[4], NT) + b_in[4:5, :])

    each(count, make_gate)
    wait_weights(1)

    def outer_copy(dest, ch):
        return remote(
            prod.at[dest, :, places(ch)], outer.at[:, channels(slot, ch)],
            o_send.at[ch], o_recv.at[ch], block * per + dest,
        )

    for ch in range(chunks):
        drain(left_in.at[:, :, places(ch)], l_recv.at[ch])
        drain(right_in.at[:, :, places(ch)], r_recv.at[ch])
        for h in range(cols_n):
            for c in range(edges[ch], edges[ch + 1]):
                lhs = left_in[:, h, c].reshape(per * count, length)
                rhs = right_in[:, h, c].reshape(length, length)
                prod[:, h, c] = dot(lhs, rhs, NT).astype(BF16).reshape(per, count, length)
        each(per - 1, lambda d: outer_copy(lax.rem(slot + 1 + d, per), ch).start())
        pltpu.make_async_copy(
            prod.at[slot, :, places(ch)], outer.at[:, channels(slot, ch)], o_recv.at[ch]
        ).start()

    for ch in range(chunks):
        drain(prod.at[:, :, places(ch)], o_recv.at[ch])

    head_t = head_w[...]
    blank = jnp.zeros((bins, width), BF16)
    spread_w = [
        jnp.concatenate([head_t if h == p else blank for h in range(packed)], axis=0)
        for p in range(packed)
    ]
    bias_row = jnp.concatenate([head_b[...]] * packed, axis=1)

    gain_col, shift_col = small[:, 5:6], small[:, 6:7]
    for b in range(spans):
        span = slice(b * lanes, (b + 1) * lanes)
        values = outer[:, :, :, span].astype(F32).reshape(width, count, lanes)
        average = jnp.sum(values, axis=0) * (1.0 / width)
        outer_f[b] = values.reshape(width * count, lanes)
        centred = values - average[None]
        inverse = lax.rsqrt(jnp.sum(centred * centred, axis=0) * (1.0 / width) + 1.0)
        for i in range(count):
            part_i = outer_f[b, pl.ds(i, width, stride=count), :]
            part_i = (part_i - average[i:i + 1, :]) * inverse[i:i + 1, :] * gain_col + shift_col
            mixed = dot(part_i.astype(BF16), wo[...], TN) + b_out[...]
            rounded = (gate[i, span, :] * mixed).astype(BF16)
            update[i, span, :] = rounded
            new_pair[i, span, :] = (pair[i, span, :].astype(F32) + rounded.astype(F32)).astype(BF16)
    for i in range(quads):
        total = bias_row
        for p in range(packed):
            total = total + dot(new_pair[p * quads + i], spread_w[p], NT)
        logit_b[:, i] = total.astype(BF16).reshape(groups, count, 128)

    def logit_copy(dest):
        return remote(
            logit_b.at[dest], logit_in.at[me],
            m_send.at[0], m_recv.at[0], dest,
        )

    logit_local = pltpu.make_async_copy(
        logit_b.at[me], logit_in.at[me], m_recv.at[0]
    )
    each(groups - 1, lambda d: logit_copy(lax.rem(me + 1 + d, groups)).start())
    logit_local.start()

    bias_col = jnp.concatenate([head_b[...], jnp.zeros((7, bins), F32)], axis=0).T[:, 0:1]
    for i in range(count):
        own_t[i] = dot(head_t, new_pair[i], NT) + bias_col
    at = lax.broadcasted_iota(jnp.int32, (length, length), 0)
    to = lax.broadcasted_iota(jnp.int32, (length, length), 1)
    fold = length // packed
    order = ((at % fold) // quads) * count + (at // fold) * quads + at % quads
    shuffle = jnp.where(order == to, 1.0, 0.0).astype(BF16)

    drain(logit_in, m_recv.at[0])
    logit_f[...] = logit_in[...].astype(F32).reshape(logit_f.shape)
    bin_id = lax.broadcasted_iota(jnp.int32, (bins, length), 0)
    for i in range(count):
        flipped = logit_f[pl.ds(i, groups * quads, stride=count), :].T
        flipped = jnp.concatenate([flipped[p * bins:(p + 1) * bins] for p in range(packed)], axis=1)
        symmetric = own_t[i] + dot(flipped.astype(BF16), shuffle)
        top = jnp.max(symmetric, axis=0, keepdims=True)
        total = top + jnp.log(jnp.sum(jnp.exp(symmetric - top), axis=0, keepdims=True))
        chosen = jnp.sum(jnp.where(bin_id == targets[i:i + 1, :], symmetric, 0.0), axis=0, keepdims=True)
        loss[i:i + 1, :] = pair_mask[i:i + 1, :] * (total - chosen)

    for ch in range(chunks):
        drain(left_in.at[pl.ds(0, per - 1), :, places(ch)], l_send.at[ch])
        drain(right_in.at[pl.ds(0, groups - 1), :, places(ch)], r_send.at[ch])
        drain(prod.at[pl.ds(0, per - 1), :, places(ch)], o_send.at[ch])
    drain(logit_in.at[pl.ds(0, groups - 1)], m_send.at[0])


def finish(update, loss, update_out, loss_out, sem):
    first = pltpu.make_async_copy(update, update_out, sem.at[0])
    second = pltpu.make_async_copy(loss, loss_out, sem.at[1])
    first.start()
    second.start()
    first.wait()
    second.wait()


def local(rows_n, cols_n, *args):
    pair, residue_mask, targets, ln_gain, ln_shift, w_in, b_in, w_out, b_out, head_w, head_b = args
    count, length, width = pair.shape
    bins = head_w.shape[1]
    groups = rows_n * cols_n
    sup = SUPER
    per = groups // sup
    share = width // per
    chunks = 2
    part, half = share // cols_n, width // cols_n
    packed = 128 // bins
    quads = count // packed
    dma = pltpu.SemaphoreType.DMA
    vmem = pl.BlockSpec(memory_space=pltpu.VMEM)
    inputs = (
        pair, residue_mask.reshape(1, length), targets, ln_gain, ln_shift,
        jnp.swapaxes(w_in, 1, 2), b_in, w_out, b_out.reshape(1, width), head_w.T,
        head_b.reshape(1, bins),
    )
    update, loss = pl.pallas_call(
        functools.partial(kernel, rows_n, cols_n, sup, chunks),
        out_shape=(
            pltpu.VMEM(pair.shape, BF16),
            pltpu.VMEM((count, length), F32),
        ),
        in_specs=[pl.BlockSpec(memory_space=pl.ANY)] * 11,
        out_specs=(vmem, vmem),
        scratch_shapes=[pltpu.VMEM(x.shape, x.dtype) for x in inputs] + [
            pltpu.VMEM((5, width, width), BF16),
            pltpu.VMEM((width, width), BF16),
            pltpu.VMEM((width, 8), F32),
            pltpu.VMEM((count, length, width), BF16),
            pltpu.VMEM((length // 128, width // cols_n * count, 128), F32),
            pltpu.VMEM((cols_n, half, count, length), BF16),
            pltpu.VMEM((cols_n, half, count, length), BF16),
            pltpu.VMEM((per, cols_n, part, count, length), BF16),
            pltpu.VMEM((groups, cols_n, part, count, length), BF16),
            pltpu.VMEM((per, cols_n, part, count, length), BF16),
            pltpu.VMEM((cols_n, half, count, length), BF16),
            pltpu.VMEM((length // 128, width * count, 128), F32),
            pltpu.VMEM((count, length, width), F32),
            pltpu.VMEM((count, length, width), BF16),
            pltpu.VMEM((groups, quads, count, 128), BF16),
            pltpu.VMEM((groups, quads, count, 128), BF16),
            pltpu.VMEM((groups * quads * count, 128), F32),
            pltpu.VMEM((count, bins, length), F32),
            dma((2, cols_n)), dma((2, cols_n)),
            dma((chunks,)), dma((chunks,)), dma((chunks,)), dma((chunks,)), dma((chunks,)), dma((chunks,)),
            dma((1,)), dma((1,)),
            dma((11,)),
        ],
        compiler_params=pltpu.CompilerParams(
            collective_id=0, has_side_effects=True, vmem_limit_bytes=60 * 1024 * 1024
        ),
    )(*inputs)
    anywhere = pl.BlockSpec(memory_space=pl.ANY)
    return pl.pallas_call(
        finish,
        out_shape=(
            jax.ShapeDtypeStruct(update.shape, update.dtype), jax.ShapeDtypeStruct(loss.shape, loss.dtype),
        ),
        in_specs=[pl.BlockSpec(memory_space=pltpu.VMEM)] * 2, compiler_params=pltpu.CompilerParams(vmem_limit_bytes=1024*1024),
        out_specs=(anywhere, anywhere),
        scratch_shapes=[dma((2,))],
    )(update, loss)


def solution(mesh):
    placed = (
        P(("ga", "row", "col"), None, None),
        P("ga"),
        P(("ga", "row", "col"), None),
        P(),
        P(),
        P(None, None, "col"),
        P(),
        P("col", None),
        P(),
        P(),
        P(),
    )
    return jax.shard_map(
        functools.partial(local, mesh.shape["row"], mesh.shape["col"]),
        mesh=mesh,
        in_specs=placed,
        out_specs=(P(("ga", "row", "col"), None, None), P(("ga", "row", "col"), None)),
        check_vma=False,
    )
```

```python
import functools

import jax
import jax.numpy as jnp
from jax import lax
from jax.experimental import pallas as pl
from jax.experimental.pallas import tpu as pltpu
from jax.sharding import PartitionSpec as P

SUPER = 2
FEW = 7
CUT = 6
F32, BF16 = jnp.float32, jnp.bfloat16
NT = (((1,), (1,)), ((), ()))
TN = (((0,), (0,)), ((), ()))


def dot(lhs, rhs, dims=(((1,), (0,)), ((), ()))):
    return lax.dot_general(lhs, rhs, dims, preferred_element_type=F32)


def kernel(
    rows_n, cols_n, sup, chunks,
    *refs,
):
    sources, (update, loss) = refs[:11], refs[11:13]
    held, rest = refs[13:24], refs[24:]
    (pair, mask, targets, ln_gain, ln_shift, w_in, b_in, w_out, b_out, head_w, head_b) = held
    (
    wt, wo, small, normed, side_f, right_b, left_b, left_in, right_in, prod, outer, outer_f, gate,
        new_pair, logit_b, logit_in, logit_f, own_t,
        w_send, w_recv, l_send, l_recv, r_send, r_recv, o_send, o_recv, m_send, m_recv,
        in_sem, far_sem,
    ) = rest
    groups = rows_n * cols_n
    count, length, width = pair.shape
    bins = head_w.shape[0]
    per = groups // sup
    share = width // per
    part = share // cols_n
    few = part * FEW // 8 if part >= 4 else part
    sizes = (few, 2 * part - few)
    edges = [[0, max(size * CUT // 8, 1), size] for size in sizes]
    half = w_in.shape[1]
    lanes = 128
    spans = length // lanes
    packed = 128 // bins
    quads = count // packed
    col = lax.axis_index("col")
    me = lax.axis_index("row") * cols_n + col
    block, slot = lax.div(me, per), lax.rem(me, per)
    plane = per // 2
    layer, place = lax.div(me, plane), lax.rem(me, plane)
    inner = lax.rem(layer + block, 2) == 1
    layers = groups // plane

    def where(peer):
        return {"row": lax.div(peer, cols_n), "col": lax.rem(peer, cols_n)}

    def remote(src, dst, send, recv, peer):
        return pltpu.make_async_remote_copy(
            src_ref=src, dst_ref=dst, send_sem=send, recv_sem=recv,
            device_id=where(peer), device_id_type=pl.DeviceIdType.MESH,
        )

    def each(n, body):
        lax.fori_loop(0, n, lambda i, c: (body(i), c)[1], 0, unroll=True)

    loads = [pltpu.make_async_copy(sources[n], held[n], in_sem.at[n]) for n in range(11)]
    for load in loads:
        load.start()
    barrier = pltpu.get_barrier_semaphore()

    def greet(d):
        peer = lax.rem(me + 1 + d, groups)
        apart = lax.div(peer, plane) - layer

        @pl.when(apart * apart < 2)
        def _():
            pl.semaphore_signal(
                barrier, inc=1, device_id=where(peer), device_id_type=pl.DeviceIdType.MESH
            )

    each(groups - 1, greet)

    def drain(ref, sem):
        pltpu.make_async_copy(ref, ref, sem).wait()


    for load in loads:
        load.wait()
    mine = pl.ds(pl.multiple_of(col * half, half), half)
    wt[:, mine, :] = w_in[...]
    wo[mine, :] = w_out[...]

    def norm_rows(i):
        values = pair[i].astype(F32)
        centred = values - jnp.mean(values, axis=-1, keepdims=True)
        spread = jnp.mean(centred * centred, axis=-1, keepdims=True)
        scaled = centred * lax.rsqrt(spread + 0.1) * ln_gain[0:1, :] + ln_shift[0:1, :]
        normed[i] = scaled.astype(BF16)

    each(count, norm_rows)

    row_mask = mask[...].astype(F32)
    lane = lax.broadcasted_iota(jnp.int32, (count, length), 1)
    sub = lax.broadcasted_iota(jnp.int32, (count, length), 0)
    own_mask = jnp.sum(jnp.where(lane == me * count + sub, row_mask, 0.0), axis=1, keepdims=True)
    pair_mask = own_mask * row_mask

    small[...] = jnp.concatenate(
        [b_in[...], ln_gain[1:2, :], ln_shift[1:2, :], jnp.zeros((1, width), F32)], axis=0
    ).T

    def weight_copies(peer_col):
        peer = me - col + peer_col
        return (
            remote(wt.at[:, mine, :], wt.at[:, mine, :], w_send.at[0, peer_col], w_recv.at[0, col], peer),
            remote(wo.at[mine, :], wo.at[mine, :], w_send.at[1, peer_col], w_recv.at[1, col], peer),
        )

    def wait_weights(which):
        for d in range(1, cols_n):
            peer_col = lax.rem(col + d, cols_n)
            theirs = pl.ds(pl.multiple_of(peer_col * half, half), half)
            ref = (wt.at[:, theirs, :], wo.at[theirs, :])[which]
            mine_ref = (wt.at[:, mine, :], wo.at[mine, :])[which]
            peer = me - col + peer_col
            remote(ref, ref, w_send.at[which, peer_col], w_recv.at[which, peer_col], peer).wait_recv()
            remote(mine_ref, mine_ref, w_send.at[which, peer_col], w_recv.at[which, peer_col], peer).wait_send()

    def make_side(first, out, span_w):
        start = pl.multiple_of(span_w * half, half)
        rows = pl.ds(start, half)
        weights = wt[first:first + 2, rows, :].reshape(2 * half, width)
        value_b, gate_b = small[rows, first:first + 1], small[rows, first + 1:first + 2]

        for i in range(count):
            both = dot(weights, normed[i], NT)
            value = jax.nn.sigmoid(both[half:] + gate_b) * (both[:half] + value_b)
            for b in range(spans):
                side_f[b, pl.ds(i, half, stride=count), :] = value[:, b * lanes:(b + 1) * lanes]
        for b in range(spans):
            span = slice(b * lanes, (b + 1) * lanes)
            masked = side_f[b].reshape(half, count, lanes) * pair_mask[:, span][None]
            out[span_w, :, :, span] = masked.astype(BF16)

    def span_of(kind, ch):
        return edges[kind][ch + 1] - edges[kind][ch]

    def whole(ch):
        return plane * (span_of(0, ch) + span_of(1, ch))

    def channels(kind, at, ch):
        return pl.ds(kind * plane * sizes[0] + at * sizes[kind] + edges[kind][ch], span_of(kind, ch))

    def places(kind, ch):
        return pl.ds(edges[kind][ch], span_of(kind, ch))

    def device(kind, part_of, at):
        return part_of * per + lax.rem(kind + part_of, 2) * plane + at

    def by_kind(body):
        pl.when(inner)(functools.partial(body, 1))
        pl.when(jnp.logical_not(inner))(functools.partial(body, 0))

    def left_copy(kind, at, ch, h):
        return remote(
            left_b.at[h, channels(kind, at, ch)], left_in.at[slot, h, places(kind, ch)],
            l_send.at[ch], l_recv.at[ch], device(kind, block, at),
        )

    def right_copy(kind, part_of, at, ch, h, way=0):
        return remote(
            right_b.at[h, channels(kind, at, ch)], right_in.at[me, h, places(kind, ch)],
            r_send.at[ch], r_recv.at[way, ch], device(kind, part_of, at),
        )

    def pass_on(ch):
        def one(d):
            piece = right_in.at[3 * block * plane + lax.rem(place + d, plane), :, places(1, ch)]
            remote(
                piece, piece, r_send.at[ch], r_recv.at[0, ch], device(1, 1 - block, place)
            ).start()

        each(plane, one)

    def send_right(kind, ch, h):
        way = kind * (1 - inner.astype(jnp.int32))

        def one(d):
            at = lax.rem(place + d, plane)

            @pl.when(device(kind, block, at) != me)
            def _():
                right_copy(kind, block, at, ch, h, way).start()

        each(plane, one)

    def send_left(kind, ch, h):
        def one(d):
            at = lax.rem(place + d, plane)

            @pl.when(device(kind, block, at) != me)
            def _():
                left_copy(kind, at, ch, h).start()

        each(plane, one)

    def send_block(ch, h):
        for kind in (1, 0):
            send_right(kind, ch, h)
            send_left(kind, ch, h)

    def send_across(kind, ch, h):
        def one(d):
            right_copy(kind, 1 - block, lax.rem(place + d, plane), ch, h).start()

        each(plane, one)

    def keep(ch):
        def own(kind):
            pltpu.make_async_copy(
                right_b.at[:, channels(kind, place, ch)], right_in.at[me, :, places(kind, ch)], r_recv.at[0, ch]
            ).start()
            pltpu.make_async_copy(
                left_b.at[:, channels(kind, place, ch)], left_in.at[slot, :, places(kind, ch)], l_recv.at[ch]
            ).start()

        by_kind(own)

    make_side(2, right_b, col)
    pl.semaphore_wait(barrier, plane * (2 + inner.astype(jnp.int32)) - 1)

    def tell(peer):
        pl.semaphore_signal(far_sem, inc=1, device_id=where(peer), device_id_type=pl.DeviceIdType.MESH)

    @pl.when(inner)
    def _():
        tell(me + plane - 2 * plane * block)

    for d in range(1, cols_n):
        for copy in weight_copies(lax.rem(col + d, cols_n)):
            copy.start()
    for turn in range(cols_n):
        h = lax.rem(col + turn, cols_n)
        if turn:
            if turn == 1:
                wait_weights(0)
            make_side(2, right_b, h)
        pl.when(inner)(functools.partial(send_across, 1, 0, h))
        pl.when(jnp.logical_not(inner))(functools.partial(send_right, 1, 0, h))
        make_side(0, left_b, h)
        send_left(1, 0, h)
        pl.when(inner)(functools.partial(send_right, 1, 0, h))
        send_left(0, 0, h)
        send_right(0, 0, h)
    keep(0)
    every = slice(None)

    @pl.when(jnp.logical_not(inner))
    def _():
        send_right(1, 1, every)

    pl.semaphore_wait(far_sem, 1)

    @pl.when(inner)
    def _():
        tell(me - plane + 2 * plane * block)
        send_across(0, 0, every)
        send_across(0, 1, every)
        send_block(1, every)

    @pl.when(jnp.logical_not(inner))
    def _():
        send_across(0, 0, every)
        send_left(1, 1, every)
        send_left(0, 1, every)
        send_right(0, 1, every)
        send_across(0, 1, every)

    keep(1)

    def make_gate(i):
        gate[i] = jax.nn.sigmoid(dot(normed[i], wt[4], NT) + b_in[4:5, :])

    each(count, make_gate)

    @pl.when(inner)
    def _():
        for ch in range(chunks):
            drain(right_in.at[pl.ds(0, plane), :, places(1, ch)], r_recv.at[1, ch])
            pass_on(ch)
            if ch == 0:
                send_across(1, 1, every)

    wait_weights(1)

    def multiply(kind):
        def outer_copy(dest, ch):
            return remote(
                prod.at[dest, :, places(kind, ch)], outer.at[:, channels(kind, place, ch)],
                o_send.at[ch], o_recv.at[ch], block * per + dest,
            )

        for ch in range(chunks):
            now = places(kind, ch)
            drain(left_in.at[:, :, now], l_recv.at[ch])
            drain(right_in.at[pl.ds(0, groups - kind * plane), :, now], r_recv.at[0, ch])
            for h in range(cols_n):
                for c in range(edges[kind][ch], edges[kind][ch + 1]):
                    lhs = left_in[:, h, c].reshape(per * count, length)
                    rhs = right_in[:, h, c].reshape(length, length)
                    prod[:, h, c] = dot(lhs, rhs, NT).astype(BF16).reshape(per, count, length)
            each(per - 1, lambda d: outer_copy(lax.rem(slot + 1 + d, per), ch).start())
            pltpu.make_async_copy(
                prod.at[slot, :, now], outer.at[:, channels(kind, place, ch)], o_recv.at[ch]
            ).start()

    by_kind(multiply)

    for ch in range(chunks):
        drain(outer.at[:, pl.ds(0, whole(ch))], o_recv.at[ch])

    head_t = head_w[...]
    blank = jnp.zeros((bins, width), BF16)
    spread_w = [
        jnp.concatenate([head_t if h == p else blank for h in range(packed)], axis=0)
        for p in range(packed)
    ]
    bias_row = jnp.concatenate([head_b[...]] * packed, axis=1)

    gain_col, shift_col = small[:, 5:6], small[:, 6:7]
    for b in range(spans):
        span = slice(b * lanes, (b + 1) * lanes)
        values = outer[:, :, :, span].astype(F32).reshape(width, count, lanes)
        average = jnp.sum(values, axis=0) * (1.0 / width)
        outer_f[b] = values.reshape(width * count, lanes)
        centred = values - average[None]
        inverse = lax.rsqrt(jnp.sum(centred * centred, axis=0) * (1.0 / width) + 1.0)
        for i in range(count):
            part_i = outer_f[b, pl.ds(i, width, stride=count), :]
            part_i = (part_i - average[i:i + 1, :]) * inverse[i:i + 1, :] * gain_col + shift_col
            mixed = dot(part_i.astype(BF16), wo[...], TN) + b_out[...]
            rounded = (gate[i, span, :] * mixed).astype(BF16)
            update[i, span, :] = rounded
            new_pair[i, span, :] = (pair[i, span, :].astype(F32) + rounded.astype(F32)).astype(BF16)
    for i in range(quads):
        total = bias_row
        for p in range(packed):
            total = total + dot(new_pair[p * quads + i], spread_w[p], NT)
        logit_b[:, i] = total.astype(BF16).reshape(groups, count, 128)

    def logit_copy(dest):
        return remote(
            logit_b.at[dest], logit_in.at[me],
            m_send.at[0], m_recv.at[0], dest,
        )

    logit_local = pltpu.make_async_copy(
        logit_b.at[me], logit_in.at[me], m_recv.at[0]
    )
    each(groups - 1, lambda d: logit_copy(lax.rem(me + 1 + d, groups)).start())
    logit_local.start()

    bias_col = jnp.concatenate([head_b[...], jnp.zeros((7, bins), F32)], axis=0).T[:, 0:1]
    for i in range(count):
        own_t[i] = dot(head_t, new_pair[i], NT) + bias_col
    at = lax.broadcasted_iota(jnp.int32, (length, length), 0)
    to = lax.broadcasted_iota(jnp.int32, (length, length), 1)
    fold = length // packed
    order = ((at % fold) // quads) * count + (at // fold) * quads + at % quads
    shuffle = jnp.where(order == to, 1.0, 0.0).astype(BF16)

    def sent(kind):
        for ch in range(chunks):
            drain(left_b.at[:, pl.ds(0, whole(ch) - span_of(kind, ch))], l_send.at[ch])
            drain(right_b.at[:, pl.ds(0, whole(ch) - span_of(kind, ch))], r_send.at[ch])
            drain(right_b.at[:, pl.ds(0, plane * span_of(0, ch))], r_send.at[ch])
            if kind:
                for _ in range(2):
                    drain(right_b.at[:, pl.ds(0, plane * span_of(1, ch))], r_send.at[ch])
            drain(prod.at[pl.ds(0, per - 1), :, places(kind, ch)], o_send.at[ch])

    by_kind(sent)

    drain(logit_in, m_recv.at[0])
    logit_f[...] = logit_in[...].astype(F32).reshape(logit_f.shape)
    bin_id = lax.broadcasted_iota(jnp.int32, (bins, length), 0)
    for i in range(count):
        flipped = logit_f[pl.ds(i, groups * quads, stride=count), :].T
        flipped = jnp.concatenate([flipped[p * bins:(p + 1) * bins] for p in range(packed)], axis=1)
        symmetric = own_t[i] + dot(flipped.astype(BF16), shuffle)
        top = jnp.max(symmetric, axis=0, keepdims=True)
        total = top + jnp.log(jnp.sum(jnp.exp(symmetric - top), axis=0, keepdims=True))
        chosen = jnp.sum(jnp.where(bin_id == targets[i:i + 1, :], symmetric, 0.0), axis=0, keepdims=True)
        loss[i:i + 1, :] = pair_mask[i:i + 1, :] * (total - chosen)

    drain(logit_in.at[pl.ds(0, groups - 1)], m_send.at[0])


def finish(update, loss, update_out, loss_out, sem):
    first = pltpu.make_async_copy(update, update_out, sem.at[0])
    second = pltpu.make_async_copy(loss, loss_out, sem.at[1])
    first.start()
    second.start()
    first.wait()
    second.wait()


def local(rows_n, cols_n, *args):
    pair, residue_mask, targets, ln_gain, ln_shift, w_in, b_in, w_out, b_out, head_w, head_b = args
    count, length, width = pair.shape
    bins = head_w.shape[1]
    groups = rows_n * cols_n
    sup = SUPER
    per = groups // sup
    share = width // per
    chunks = 2
    part, half = share // cols_n, width // cols_n
    most = 2 * part - (part * FEW // 8 if part >= 4 else part)
    packed = 128 // bins
    quads = count // packed
    dma = pltpu.SemaphoreType.DMA
    vmem = pl.BlockSpec(memory_space=pltpu.VMEM)
    inputs = (
        pair, residue_mask.reshape(1, length), targets, ln_gain, ln_shift,
        jnp.swapaxes(w_in, 1, 2), b_in, w_out, b_out.reshape(1, width), head_w.T,
        head_b.reshape(1, bins),
    )
    update, loss = pl.pallas_call(
        functools.partial(kernel, rows_n, cols_n, sup, chunks),
        out_shape=(
            pltpu.VMEM(pair.shape, BF16),
            pltpu.VMEM((count, length), F32),
        ),
        in_specs=[pl.BlockSpec(memory_space=pl.ANY)] * 11,
        out_specs=(vmem, vmem),
        scratch_shapes=[pltpu.VMEM(x.shape, x.dtype) for x in inputs] + [
            pltpu.VMEM((5, width, width), BF16),
            pltpu.VMEM((width, width), BF16),
            pltpu.VMEM((width, 8), F32),
            pltpu.VMEM((count, length, width), BF16),
            pltpu.VMEM((length // 128, width // cols_n * count, 128), F32),
            pltpu.VMEM((cols_n, half, count, length), BF16),
            pltpu.VMEM((cols_n, half, count, length), BF16),
            pltpu.VMEM((per, cols_n, most, count, length), BF16),
            pltpu.VMEM((groups, cols_n, most, count, length), BF16),
            pltpu.VMEM((per, cols_n, most, count, length), BF16),
            pltpu.VMEM((cols_n, half, count, length), BF16),
            pltpu.VMEM((length // 128, width * count, 128), F32),
            pltpu.VMEM((count, length, width), F32),
            pltpu.VMEM((count, length, width), BF16),
            pltpu.VMEM((groups, quads, count, 128), BF16),
            pltpu.VMEM((groups, quads, count, 128), BF16),
            pltpu.VMEM((groups * quads * count, 128), F32),
            pltpu.VMEM((count, bins, length), F32),
            dma((2, cols_n)), dma((2, cols_n)),
            dma((chunks,)), dma((chunks,)), dma((chunks,)), dma((2, chunks)), dma((chunks,)), dma((chunks,)),
            dma((1,)), dma((1,)),
            dma((11,)), pltpu.SemaphoreType.REGULAR,
        ],
        compiler_params=pltpu.CompilerParams(
            collective_id=0, has_side_effects=True, vmem_limit_bytes=60 * 1024 * 1024
        ),
    )(*inputs)
    anywhere = pl.BlockSpec(memory_space=pl.ANY)
    return pl.pallas_call(
        finish,
        out_shape=(
            jax.ShapeDtypeStruct(update.shape, update.dtype), jax.ShapeDtypeStruct(loss.shape, loss.dtype),
        ),
        in_specs=[pl.BlockSpec(memory_space=pltpu.VMEM)] * 2, compiler_params=pltpu.CompilerParams(vmem_limit_bytes=1024*1024),
        out_specs=(anywhere, anywhere),
        scratch_shapes=[dma((2,))],
    )(update, loss)


def solution(mesh):
    placed = (
        P(("ga", "row", "col"), None, None),
        P("ga"),
        P(("ga", "row", "col"), None),
        P(),
        P(),
        P(None, None, "col"),
        P(),
        P("col", None),
        P(),
        P(),
        P(),
    )
    return jax.shard_map(
        functools.partial(local, mesh.shape["row"], mesh.shape["col"]),
        mesh=mesh,
        in_specs=placed,
        out_specs=(P(("ga", "row", "col"), None, None), P(("ga", "row", "col"), None)),
        check_vma=False,
    )
```

```python
import functools

import jax
import jax.numpy as jnp
from jax import lax
from jax.experimental import pallas as pl
from jax.experimental.pallas import tpu as pltpu
from jax.sharding import PartitionSpec as P

SUPER = 2
FEW = 7
CUT = 6
F32, BF16 = jnp.float32, jnp.bfloat16
NT = (((1,), (1,)), ((), ()))
TN = (((0,), (0,)), ((), ()))


def dot(lhs, rhs, dims=(((1,), (0,)), ((), ()))):
    return lax.dot_general(lhs, rhs, dims, preferred_element_type=F32)


def kernel(
    rows_n, cols_n, sup, chunks,
    *refs,
):
    sources, (update, loss) = refs[:11], refs[11:13]
    held, rest = refs[13:24], refs[24:]
    (pair, mask, targets, ln_gain, ln_shift, w_in, b_in, w_out, b_out, head_w, head_b) = held
    (
    wt, wo, small, normed, side_f, right_b, left_b, left_in, right_in, prod, outer, outer_f, gate,
        new_pair, logit_b, logit_in, logit_f, own_t,
        w_send, w_recv, l_send, l_recv, r_send, r_recv, o_send, o_recv, m_send, m_recv,
        in_sem, far_sem, spread_w, shuffle,
    ) = rest
    groups = rows_n * cols_n
    count, length, width = pair.shape
    bins = head_w.shape[0]
    per = groups // sup
    share = width // per
    part = share // cols_n
    few = part * FEW // 8 if part >= 4 else part
    sizes = (few, 2 * part - few)
    edges = [[0, max(size * CUT // 8, 1), size] for size in sizes]
    half = w_in.shape[1]
    lanes = 128
    spans = length // lanes
    packed = 128 // bins
    quads = count // packed
    col = lax.axis_index("col")
    me = lax.axis_index("row") * cols_n + col
    block, slot = lax.div(me, per), lax.rem(me, per)
    plane = per // 2
    layer, place = lax.div(me, plane), lax.rem(me, plane)
    inner = lax.rem(layer + block, 2) == 1
    layers = groups // plane

    def where(peer):
        return {"row": lax.div(peer, cols_n), "col": lax.rem(peer, cols_n)}

    def remote(src, dst, send, recv, peer):
        return pltpu.make_async_remote_copy(
            src_ref=src, dst_ref=dst, send_sem=send, recv_sem=recv,
            device_id=where(peer), device_id_type=pl.DeviceIdType.MESH,
        )

    def each(n, body):
        lax.fori_loop(0, n, lambda i, c: (body(i), c)[1], 0, unroll=True)

    loads = [pltpu.make_async_copy(sources[n], held[n], in_sem.at[n]) for n in range(11)]
    for load in loads:
        load.start()
    barrier = pltpu.get_barrier_semaphore()

    def greet(d):
        peer = lax.rem(me + 1 + d, groups)
        apart = lax.div(peer, plane) - layer

        @pl.when(apart * apart < 2)
        def _():
            pl.semaphore_signal(
                barrier, inc=1, device_id=where(peer), device_id_type=pl.DeviceIdType.MESH
            )

    each(groups - 1, greet)

    def drain(ref, sem):
        pltpu.make_async_copy(ref, ref, sem).wait()


    for load in loads:
        load.wait()
    mine = pl.ds(pl.multiple_of(col * half, half), half)
    wt[:, mine, :] = w_in[...]
    wo[mine, :] = w_out[...]

    def norm_rows(i):
        values = pair[i].astype(F32)
        centred = values - jnp.mean(values, axis=-1, keepdims=True)
        spread = jnp.mean(centred * centred, axis=-1, keepdims=True)
        scaled = centred * lax.rsqrt(spread + 0.1) * ln_gain[0:1, :] + ln_shift[0:1, :]
        normed[i] = scaled.astype(BF16)

    each(count, norm_rows)

    row_mask = mask[...].astype(F32)
    lane = lax.broadcasted_iota(jnp.int32, (count, length), 1)
    sub = lax.broadcasted_iota(jnp.int32, (count, length), 0)
    own_mask = jnp.sum(jnp.where(lane == me * count + sub, row_mask, 0.0), axis=1, keepdims=True)
    pair_mask = own_mask * row_mask

    small[...] = jnp.concatenate(
        [b_in[...], ln_gain[1:2, :], ln_shift[1:2, :], jnp.zeros((1, width), F32)], axis=0
    ).T

    def weight_copies(peer_col):
        peer = me - col + peer_col
        return (
            remote(wt.at[:, mine, :], wt.at[:, mine, :], w_send.at[0, peer_col], w_recv.at[0, col], peer),
            remote(wo.at[mine, :], wo.at[mine, :], w_send.at[1, peer_col], w_recv.at[1, col], peer),
        )

    def wait_weights(which):
        for d in range(1, cols_n):
            peer_col = lax.rem(col + d, cols_n)
            theirs = pl.ds(pl.multiple_of(peer_col * half, half), half)
            ref = (wt.at[:, theirs, :], wo.at[theirs, :])[which]
            mine_ref = (wt.at[:, mine, :], wo.at[mine, :])[which]
            peer = me - col + peer_col
            remote(ref, ref, w_send.at[which, peer_col], w_recv.at[which, peer_col], peer).wait_recv()
            remote(mine_ref, mine_ref, w_send.at[which, peer_col], w_recv.at[which, peer_col], peer).wait_send()

    def make_side(first, out, span_w):
        start = pl.multiple_of(span_w * half, half)
        rows = pl.ds(start, half)
        weights = wt[first:first + 2, rows, :].reshape(2 * half, width)
        value_b, gate_b = small[rows, first:first + 1], small[rows, first + 1:first + 2]

        for i in range(count):
            both = dot(weights, normed[i], NT)
            value = jax.nn.sigmoid(both[half:] + gate_b) * (both[:half] + value_b)
            for b in range(spans):
                side_f[b, pl.ds(i, half, stride=count), :] = value[:, b * lanes:(b + 1) * lanes]
        for b in range(spans):
            span = slice(b * lanes, (b + 1) * lanes)
            masked = side_f[b].reshape(half, count, lanes) * pair_mask[:, span][None]
            out[span_w, :, :, span] = masked.astype(BF16)

    def span_of(kind, ch):
        return edges[kind][ch + 1] - edges[kind][ch]

    def whole(ch):
        return plane * (span_of(0, ch) + span_of(1, ch))

    def channels(kind, at, ch):
        return pl.ds(kind * plane * sizes[0] + at * sizes[kind] + edges[kind][ch], span_of(kind, ch))

    def places(kind, ch):
        return pl.ds(edges[kind][ch], span_of(kind, ch))

    def device(kind, part_of, at):
        return part_of * per + lax.rem(kind + part_of, 2) * plane + at

    def by_kind(body):
        pl.when(inner)(functools.partial(body, 1))
        pl.when(jnp.logical_not(inner))(functools.partial(body, 0))

    def left_copy(kind, at, ch, h):
        return remote(
            left_b.at[h, channels(kind, at, ch)], left_in.at[slot, h, places(kind, ch)],
            l_send.at[ch], l_recv.at[ch], device(kind, block, at),
        )

    def right_copy(kind, part_of, at, ch, h, way=0):
        return remote(
            right_b.at[h, channels(kind, at, ch)], right_in.at[me, h, places(kind, ch)],
            r_send.at[ch], r_recv.at[way, ch], device(kind, part_of, at),
        )

    def pass_on(ch):
        def one(d):
            piece = right_in.at[3 * block * plane + lax.rem(place + d, plane), :, places(1, ch)]
            remote(
                piece, piece, r_send.at[ch], r_recv.at[0, ch], device(1, 1 - block, place)
            ).start()

        each(plane, one)

    def send_right(kind, ch, h):
        way = kind * (1 - inner.astype(jnp.int32))

        def one(d):
            at = lax.rem(place + d, plane)

            @pl.when(device(kind, block, at) != me)
            def _():
                right_copy(kind, block, at, ch, h, way).start()

        each(plane, one)

    def send_left(kind, ch, h):
        def one(d):
            at = lax.rem(place + d, plane)

            @pl.when(device(kind, block, at) != me)
            def _():
                left_copy(kind, at, ch, h).start()

        each(plane, one)

    def send_block(ch, h):
        for kind in (1, 0):
            send_right(kind, ch, h)
            send_left(kind, ch, h)

    def send_across(kind, ch, h):
        def one(d):
            right_copy(kind, 1 - block, lax.rem(place + d, plane), ch, h).start()

        each(plane, one)

    def keep(ch):
        def own(kind):
            pltpu.make_async_copy(
                right_b.at[:, channels(kind, place, ch)], right_in.at[me, :, places(kind, ch)], r_recv.at[0, ch]
            ).start()
            pltpu.make_async_copy(
                left_b.at[:, channels(kind, place, ch)], left_in.at[slot, :, places(kind, ch)], l_recv.at[ch]
            ).start()

        by_kind(own)

    make_side(2, right_b, col)
    pl.semaphore_wait(barrier, plane * (2 + inner.astype(jnp.int32)) - 1)

    def tell(peer):
        pl.semaphore_signal(far_sem, inc=1, device_id=where(peer), device_id_type=pl.DeviceIdType.MESH)

    @pl.when(inner)
    def _():
        tell(me + plane - 2 * plane * block)

    for d in range(1, cols_n):
        for copy in weight_copies(lax.rem(col + d, cols_n)):
            copy.start()
    for turn in range(cols_n):
        h = lax.rem(col + turn, cols_n)
        if turn:
            if turn == 1:
                wait_weights(0)
            make_side(2, right_b, h)
        pl.when(inner)(functools.partial(send_across, 1, 0, h))
        pl.when(jnp.logical_not(inner))(functools.partial(send_right, 1, 0, h))
        make_side(0, left_b, h)
        send_left(1, 0, h)
        pl.when(inner)(functools.partial(send_right, 1, 0, h))
        send_left(0, 0, h)
        send_right(0, 0, h)
    keep(0)
    every = slice(None)

    @pl.when(jnp.logical_not(inner))
    def _():
        send_right(1, 1, every)

    pl.semaphore_wait(far_sem, 1)

    @pl.when(inner)
    def _():
        tell(me - plane + 2 * plane * block)
        send_across(0, 0, every)
        send_across(0, 1, every)
        send_block(1, every)

    @pl.when(jnp.logical_not(inner))
    def _():
        send_across(0, 0, every)
        send_left(1, 1, every)
        send_left(0, 1, every)
        send_right(0, 1, every)
        send_across(0, 1, every)

    keep(1)

    def make_gate(i):
        gate[i] = jax.nn.sigmoid(dot(normed[i], wt[4], NT) + b_in[4:5, :])

    each(count, make_gate)

    @pl.when(inner)
    def _():
        for ch in range(chunks):
            drain(right_in.at[pl.ds(0, plane), :, places(1, ch)], r_recv.at[1, ch])
            pass_on(ch)
            if ch == 0:
                send_across(1, 1, every)

    wait_weights(1)

    head_t = head_w[...]
    spread_w[...] = jnp.zeros(spread_w.shape, BF16)
    for p in range(packed):
        spread_w[p, p * bins:(p + 1) * bins, :] = head_t
    bias_row = jnp.concatenate([head_b[...]] * packed, axis=1)

    at = lax.broadcasted_iota(jnp.int32, (length, length), 0)
    to = lax.broadcasted_iota(jnp.int32, (length, length), 1)
    fold = length // packed
    order = ((at % fold) // quads) * count + (at // fold) * quads + at % quads
    shuffle[...] = jnp.where(order == to, 1.0, 0.0).astype(BF16)

    def multiply(kind):
        def outer_copy(dest, ch):
            return remote(
                prod.at[dest, :, places(kind, ch)], outer.at[:, channels(kind, place, ch)],
                o_send.at[ch], o_recv.at[ch], block * per + dest,
            )

        for ch in range(chunks):
            now = places(kind, ch)
            drain(left_in.at[:, :, now], l_recv.at[ch])
            drain(right_in.at[pl.ds(0, groups - kind * plane), :, now], r_recv.at[0, ch])
            for h in range(cols_n):
                for c in range(edges[kind][ch], edges[kind][ch + 1]):
                    lhs = left_in[:, h, c].reshape(per * count, length)
                    rhs = right_in[:, h, c].reshape(length, length)
                    prod[:, h, c] = dot(lhs, rhs, NT).astype(BF16).reshape(per, count, length)
            each(per - 1, lambda d: outer_copy(lax.rem(slot + 1 + d, per), ch).start())
            pltpu.make_async_copy(
                prod.at[slot, :, now], outer.at[:, channels(kind, place, ch)], o_recv.at[ch]
            ).start()

    by_kind(multiply)

    def pieces(ch):
        for kind in range(2):
            for at in range(plane):
                start = kind * plane * sizes[0] + at * sizes[kind] + edges[kind][ch]
                yield start, start + span_of(kind, ch)

    stats = [None] * spans
    for ch in range(chunks):
        drain(outer.at[:, pl.ds(0, whole(ch))], o_recv.at[ch])
        if not whole(ch):
            continue
        for b in range(spans):
            amount = cols_n * whole(ch)
            span = slice(b * lanes, (b + 1) * lanes)
            loaded, added = [], 0.0
            for h in range(cols_n):
                for start, stop in pieces(ch):
                    values = outer[h, start:stop, :, span].astype(F32)
                    rows = slice((h * half + start) * count, (h * half + stop) * count)
                    outer_f[b, rows, :] = values.reshape((stop - start) * count, lanes)
                    added = added + jnp.sum(values, axis=0)
                    loaded.append((h, start, stop))
            middle, scatter = added * (1.0 / amount), 0.0
            for h, start, stop in loaded:
                rows = slice((h * half + start) * count, (h * half + stop) * count)
                centred = outer_f[b, rows, :].reshape(stop - start, count, lanes) - middle[None]
                scatter = scatter + jnp.sum(centred * centred, axis=0)
            if stats[b] is not None:
                before, mean_b, scatter_b = stats[b]
                apart = middle - mean_b
                scatter = scatter_b + scatter + apart * apart * (before * amount / (before + amount))
                middle = mean_b + apart * (amount / (before + amount))
                amount = before + amount
            stats[b] = (amount, middle, scatter)

    gain_col, shift_col = small[:, 5:6], small[:, 6:7]
    for b in range(spans):
        span = slice(b * lanes, (b + 1) * lanes)
        average = stats[b][1]
        inverse = lax.rsqrt(stats[b][2] * (1.0 / width) + 1.0)
        for i in range(count):
            part_i = outer_f[b, pl.ds(i, width, stride=count), :]
            part_i = (part_i - average[i:i + 1, :]) * inverse[i:i + 1, :] * gain_col + shift_col
            mixed = dot(part_i.astype(BF16), wo[...], TN) + b_out[...]
            rounded = (gate[i, span, :] * mixed).astype(BF16)
            update[i, span, :] = rounded
            new_pair[i, span, :] = (pair[i, span, :].astype(F32) + rounded.astype(F32)).astype(BF16)
    for i in range(quads):
        total = bias_row
        for p in range(packed):
            total = total + dot(new_pair[p * quads + i], spread_w[p], NT)
        logit_b[:, i] = total.astype(BF16).reshape(groups, count, 128)

    def logit_copy(dest):
        return remote(
            logit_b.at[dest], logit_in.at[me],
            m_send.at[0], m_recv.at[layer], dest,
        )

    logit_local = pltpu.make_async_copy(
        logit_b.at[me], logit_in.at[me], m_recv.at[layer]
    )
    each(groups - 1, lambda d: logit_copy(lax.rem(me + 1 + d, groups)).start())
    logit_local.start()

    bias_col = jnp.concatenate([head_b[...], jnp.zeros((7, bins), F32)], axis=0).T[:, 0:1]
    for i in range(count):
        own_t[i] = dot(head_t, new_pair[i], NT) + bias_col
    def sent(kind):
        for ch in range(chunks):
            drain(left_b.at[:, pl.ds(0, whole(ch) - span_of(kind, ch))], l_send.at[ch])
            drain(right_b.at[:, pl.ds(0, whole(ch) - span_of(kind, ch))], r_send.at[ch])
            drain(right_b.at[:, pl.ds(0, plane * span_of(0, ch))], r_send.at[ch])
            if kind:
                for _ in range(2):
                    drain(right_b.at[:, pl.ds(0, plane * span_of(1, ch))], r_send.at[ch])
            drain(prod.at[pl.ds(0, per - 1), :, places(kind, ch)], o_send.at[ch])

    by_kind(sent)

    tall = plane * quads * count
    for d in range(layers):
        at = lax.rem(layer + d, layers)
        some = logit_in.at[pl.ds(at * plane, plane)]
        drain(some, m_recv.at[at])
        logit_f[pl.ds(pl.multiple_of(at * tall, tall), tall), :] = some[...].astype(F32).reshape(tall, packed * bins)
    bin_id = lax.broadcasted_iota(jnp.int32, (bins, length), 0)
    for i in range(count):
        flipped = logit_f[pl.ds(i, groups * quads, stride=count), :].T
        flipped = jnp.concatenate([flipped[p * bins:(p + 1) * bins] for p in range(packed)], axis=1)
        symmetric = own_t[i] + dot(flipped.astype(BF16), shuffle[...])
        top = jnp.max(symmetric, axis=0, keepdims=True)
        total = top + jnp.log(jnp.sum(jnp.exp(symmetric - top), axis=0, keepdims=True))
        chosen = jnp.sum(jnp.where(bin_id == targets[i:i + 1, :], symmetric, 0.0), axis=0, keepdims=True)
        loss[i:i + 1, :] = pair_mask[i:i + 1, :] * (total - chosen)

    drain(logit_in.at[pl.ds(0, groups - 1)], m_send.at[0])


def finish(update, loss, update_out, loss_out, sem):
    first = pltpu.make_async_copy(update, update_out, sem.at[0])
    second = pltpu.make_async_copy(loss, loss_out, sem.at[1])
    first.start()
    second.start()
    first.wait()
    second.wait()


def local(rows_n, cols_n, *args):
    pair, residue_mask, targets, ln_gain, ln_shift, w_in, b_in, w_out, b_out, head_w, head_b = args
    count, length, width = pair.shape
    bins = head_w.shape[1]
    groups = rows_n * cols_n
    sup = SUPER
    per = groups // sup
    share = width // per
    chunks = 2
    part, half = share // cols_n, width // cols_n
    most = 2 * part - (part * FEW // 8 if part >= 4 else part)
    packed = 128 // bins
    quads = count // packed
    dma = pltpu.SemaphoreType.DMA
    vmem = pl.BlockSpec(memory_space=pltpu.VMEM)
    inputs = (
        pair, residue_mask.reshape(1, length), targets, ln_gain, ln_shift,
        jnp.swapaxes(w_in, 1, 2), b_in, w_out, b_out.reshape(1, width), head_w.T,
        head_b.reshape(1, bins),
    )
    update, loss = pl.pallas_call(
        functools.partial(kernel, rows_n, cols_n, sup, chunks),
        out_shape=(
            pltpu.VMEM(pair.shape, BF16),
            pltpu.VMEM((count, length), F32),
        ),
        in_specs=[pl.BlockSpec(memory_space=pl.ANY)] * 11,
        out_specs=(vmem, vmem),
        scratch_shapes=[pltpu.VMEM(x.shape, x.dtype) for x in inputs] + [
            pltpu.VMEM((5, width, width), BF16),
            pltpu.VMEM((width, width), BF16),
            pltpu.VMEM((width, 8), F32),
            pltpu.VMEM((count, length, width), BF16),
            pltpu.VMEM((length // 128, width // cols_n * count, 128), F32),
            pltpu.VMEM((cols_n, half, count, length), BF16),
            pltpu.VMEM((cols_n, half, count, length), BF16),
            pltpu.VMEM((per, cols_n, most, count, length), BF16),
            pltpu.VMEM((groups, cols_n, most, count, length), BF16),
            pltpu.VMEM((per, cols_n, most, count, length), BF16),
            pltpu.VMEM((cols_n, half, count, length), BF16),
            pltpu.VMEM((length // 128, width * count, 128), F32),
            pltpu.VMEM((count, length, width), F32),
            pltpu.VMEM((count, length, width), BF16),
            pltpu.VMEM((groups, quads, count, 128), BF16),
            pltpu.VMEM((groups, quads, count, 128), BF16),
            pltpu.VMEM((groups * quads * count, 128), F32),
            pltpu.VMEM((count, bins, length), F32),
            dma((2, cols_n)), dma((2, cols_n)),
            dma((chunks,)), dma((chunks,)), dma((chunks,)), dma((2, chunks)), dma((chunks,)), dma((chunks,)),
            dma((1,)), dma((groups // (per // 2),)),
            dma((11,)), pltpu.SemaphoreType.REGULAR,
            pltpu.VMEM((packed, 128, width), BF16), pltpu.VMEM((length, length), BF16),
        ],
        compiler_params=pltpu.CompilerParams(
            collective_id=0, has_side_effects=True, vmem_limit_bytes=60 * 1024 * 1024
        ),
    )(*inputs)
    anywhere = pl.BlockSpec(memory_space=pl.ANY)
    return pl.pallas_call(
        finish,
        out_shape=(
            jax.ShapeDtypeStruct(update.shape, update.dtype), jax.ShapeDtypeStruct(loss.shape, loss.dtype),
        ),
        in_specs=[pl.BlockSpec(memory_space=pltpu.VMEM)] * 2, compiler_params=pltpu.CompilerParams(vmem_limit_bytes=1024*1024),
        out_specs=(anywhere, anywhere),
        scratch_shapes=[dma((2,))],
    )(update, loss)


def solution(mesh):
    placed = (
        P(("ga", "row", "col"), None, None),
        P("ga"),
        P(("ga", "row", "col"), None),
        P(),
        P(),
        P(None, None, "col"),
        P(),
        P("col", None),
        P(),
        P(),
        P(),
    )
    return jax.shard_map(
        functools.partial(local, mesh.shape["row"], mesh.shape["col"]),
        mesh=mesh,
        in_specs=placed,
        out_specs=(P(("ga", "row", "col"), None, None), P(("ga", "row", "col"), None)),
        check_vma=False,
    )
```

```python
import functools

import jax
import jax.numpy as jnp
from jax import lax
from jax.experimental import pallas as pl
from jax.experimental.pallas import tpu as pltpu
from jax.sharding import PartitionSpec as P

SUPER = 2
FEW = 7
CUT = 6
F32, BF16 = jnp.float32, jnp.bfloat16
NT = (((1,), (1,)), ((), ()))
TN = (((0,), (0,)), ((), ()))


def dot(lhs, rhs, dims=(((1,), (0,)), ((), ()))):
    return lax.dot_general(lhs, rhs, dims, preferred_element_type=F32)


def kernel(
    rows_n, cols_n, sup, chunks,
    *refs,
):
    sources, (update, loss) = refs[:11], refs[11:13]
    held, rest = refs[13:24], refs[24:]
    (pair, mask, targets, ln_gain, ln_shift, w_in, b_in, w_out, b_out, head_w, head_b) = held
    (
    wt, wo, small, normed, side_f, right_b, left_b, left_in, right_in, prod, outer, outer_f, gate,
        new_pair, logit_b, logit_in, logit_f, own_t,
        sent_sem, w_recv, l_recv, r_recv, o_recv, m_recv,
        in_sem, far_sem, spread_w, shuffle,
    ) = rest
    groups = rows_n * cols_n
    count, length, width = pair.shape
    bins = head_w.shape[0]
    per = groups // sup
    share = width // per
    part = share // cols_n
    few = part * FEW // 8 if part >= 4 else part
    sizes = (few, 2 * part - few)
    edges = [[0, max(size * CUT // 8, 1), size] for size in sizes]
    half = w_in.shape[1]
    lanes = 128
    spans = length // lanes
    packed = 128 // bins
    quads = count // packed
    col = lax.axis_index("col")
    me = lax.axis_index("row") * cols_n + col
    block, slot = lax.div(me, per), lax.rem(me, per)
    plane = per // 2
    layer, place = lax.div(me, plane), lax.rem(me, plane)
    inner = lax.rem(layer + block, 2) == 1
    layers = groups // plane

    def where(peer):
        return {"row": lax.div(peer, cols_n), "col": lax.rem(peer, cols_n)}

    def remote(src, dst, send, recv, peer):
        return pltpu.make_async_remote_copy(
            src_ref=src, dst_ref=dst, send_sem=send, recv_sem=recv,
            device_id=where(peer), device_id_type=pl.DeviceIdType.MESH,
        )

    def each(n, body):
        lax.fori_loop(0, n, lambda i, c: (body(i), c)[1], 0, unroll=True)

    loads = [pltpu.make_async_copy(sources[n], held[n], in_sem.at[0]) for n in range(11)]
    for load in loads:
        load.start()
    barrier = pltpu.get_barrier_semaphore()

    def greet(d):
        peer = lax.rem(me + 1 + d, groups)
        apart = lax.div(peer, plane) - layer

        @pl.when(apart * apart < 2)
        def _():
            pl.semaphore_signal(
                barrier, inc=1, device_id=where(peer), device_id_type=pl.DeviceIdType.MESH
            )

    each(groups - 1, greet)

    def drain(ref, sem):
        pltpu.make_async_copy(ref, ref, sem).wait()


    for load in loads:
        load.wait()
    mine = pl.ds(pl.multiple_of(col * half, half), half)
    wt[:, mine, :] = w_in[...]
    wo[mine, :] = w_out[...]

    def norm_rows(i):
        values = pair[i].astype(F32)
        centred = values - jnp.mean(values, axis=-1, keepdims=True)
        spread = jnp.mean(centred * centred, axis=-1, keepdims=True)
        scaled = centred * lax.rsqrt(spread + 0.1) * ln_gain[0:1, :] + ln_shift[0:1, :]
        normed[i] = scaled.astype(BF16)

    each(count, norm_rows)

    row_mask = mask[...].astype(F32)
    lane = lax.broadcasted_iota(jnp.int32, (count, length), 1)
    sub = lax.broadcasted_iota(jnp.int32, (count, length), 0)
    own_mask = jnp.sum(jnp.where(lane == me * count + sub, row_mask, 0.0), axis=1, keepdims=True)
    pair_mask = own_mask * row_mask

    small[...] = jnp.concatenate(
        [b_in[...], ln_gain[1:2, :], ln_shift[1:2, :], jnp.zeros((1, width), F32)], axis=0
    ).T

    def weight_copies(peer_col):
        peer = me - col + peer_col
        return (
            remote(wt.at[:, mine, :], wt.at[:, mine, :], sent_sem.at[0], w_recv.at[0], peer),
            remote(wo.at[mine, :], wo.at[mine, :], sent_sem.at[0], w_recv.at[1], peer),
        )

    def wait_weights(which):
        for d in range(1, cols_n):
            peer_col = lax.rem(col + d, cols_n)
            theirs = pl.ds(pl.multiple_of(peer_col * half, half), half)
            ref = (wt.at[:, theirs, :], wo.at[theirs, :])[which]
            drain(ref, w_recv.at[which])

    def make_side(first, out, span_w):
        start = pl.multiple_of(span_w * half, half)
        rows = pl.ds(start, half)
        weights = wt[first:first + 2, rows, :].reshape(2 * half, width)
        value_b, gate_b = small[rows, first:first + 1], small[rows, first + 1:first + 2]

        for i in range(count):
            both = dot(weights, normed[i], NT)
            value = jax.nn.sigmoid(both[half:] + gate_b) * (both[:half] + value_b)
            for b in range(spans):
                side_f[b, pl.ds(i, half, stride=count), :] = value[:, b * lanes:(b + 1) * lanes]
        for b in range(spans):
            span = slice(b * lanes, (b + 1) * lanes)
            masked = side_f[b].reshape(half, count, lanes) * pair_mask[:, span][None]
            out[span_w, :, :, span] = masked.astype(BF16)

    def span_of(kind, ch):
        return edges[kind][ch + 1] - edges[kind][ch]

    def whole(ch):
        return plane * (span_of(0, ch) + span_of(1, ch))

    def channels(kind, at, ch):
        return pl.ds(kind * plane * sizes[0] + at * sizes[kind] + edges[kind][ch], span_of(kind, ch))

    def places(kind, ch):
        return pl.ds(edges[kind][ch], span_of(kind, ch))

    def device(kind, part_of, at):
        return part_of * per + lax.rem(kind + part_of, 2) * plane + at

    def by_kind(body):
        pl.when(inner)(functools.partial(body, 1))
        pl.when(jnp.logical_not(inner))(functools.partial(body, 0))

    def left_copy(kind, at, ch, h):
        return remote(
            left_b.at[h, channels(kind, at, ch)], left_in.at[slot, h, places(kind, ch)],
            sent_sem.at[0], l_recv.at[ch], device(kind, block, at),
        )

    def right_copy(kind, part_of, at, ch, h, way=0):
        return remote(
            right_b.at[h, channels(kind, at, ch)], right_in.at[me, h, places(kind, ch)],
            sent_sem.at[0], r_recv.at[way, ch], device(kind, part_of, at),
        )

    def pass_on(ch):
        def one(d):
            piece = right_in.at[3 * block * plane + lax.rem(place + d, plane), :, places(1, ch)]
            remote(
                piece, piece, sent_sem.at[0], r_recv.at[0, ch], device(1, 1 - block, place)
            ).start()

        each(plane, one)

    def send_right(kind, ch, h):
        way = kind * (1 - inner.astype(jnp.int32))

        def one(d):
            at = lax.rem(place + d, plane)

            @pl.when(device(kind, block, at) != me)
            def _():
                right_copy(kind, block, at, ch, h, way).start()

        each(plane, one)

    def send_left(kind, ch, h):
        def one(d):
            at = lax.rem(place + d, plane)

            @pl.when(device(kind, block, at) != me)
            def _():
                left_copy(kind, at, ch, h).start()

        each(plane, one)

    def send_block(ch, h):
        for kind in (1, 0):
            send_right(kind, ch, h)
            send_left(kind, ch, h)

    def send_across(kind, ch, h):
        def one(d):
            right_copy(kind, 1 - block, lax.rem(place + d, plane), ch, h).start()

        each(plane, one)

    def keep(ch):
        def own(kind):
            pltpu.make_async_copy(
                right_b.at[:, channels(kind, place, ch)], right_in.at[me, :, places(kind, ch)], r_recv.at[0, ch]
            ).start()
            pltpu.make_async_copy(
                left_b.at[:, channels(kind, place, ch)], left_in.at[slot, :, places(kind, ch)], l_recv.at[ch]
            ).start()

        by_kind(own)

    make_side(2, right_b, col)
    pl.semaphore_wait(barrier, plane * (2 + inner.astype(jnp.int32)) - 1)

    def tell(peer):
        pl.semaphore_signal(far_sem, inc=1, device_id=where(peer), device_id_type=pl.DeviceIdType.MESH)

    @pl.when(inner)
    def _():
        tell(me + plane - 2 * plane * block)

    for d in range(1, cols_n):
        for copy in weight_copies(lax.rem(col + d, cols_n)):
            copy.start()
    for turn in range(cols_n):
        h = lax.rem(col + turn, cols_n)
        if turn:
            if turn == 1:
                wait_weights(0)
            make_side(2, right_b, h)
        pl.when(inner)(functools.partial(send_across, 1, 0, h))
        pl.when(jnp.logical_not(inner))(functools.partial(send_right, 1, 0, h))
        make_side(0, left_b, h)
        send_left(1, 0, h)
        pl.when(inner)(functools.partial(send_right, 1, 0, h))
        send_left(0, 0, h)
        send_right(0, 0, h)
    keep(0)
    every = slice(None)

    @pl.when(jnp.logical_not(inner))
    def _():
        send_right(1, 1, every)

    pl.semaphore_wait(far_sem, 1)

    @pl.when(inner)
    def _():
        tell(me - plane + 2 * plane * block)
        send_across(0, 0, every)
        send_across(0, 1, every)
        send_block(1, every)

    @pl.when(jnp.logical_not(inner))
    def _():
        send_across(0, 0, every)
        send_left(1, 1, every)
        send_left(0, 1, every)
        send_right(0, 1, every)
        send_across(0, 1, every)

    keep(1)

    def make_gate(i):
        gate[i] = jax.nn.sigmoid(dot(normed[i], wt[4], NT) + b_in[4:5, :])

    each(count, make_gate)

    @pl.when(inner)
    def _():
        for ch in range(chunks):
            drain(right_in.at[pl.ds(0, plane), :, places(1, ch)], r_recv.at[1, ch])
            pass_on(ch)
            if ch == 0:
                send_across(1, 1, every)

    wait_weights(1)

    head_t = head_w[...]
    spread_w[...] = jnp.zeros(spread_w.shape, BF16)
    for p in range(packed):
        spread_w[p, p * bins:(p + 1) * bins, :] = head_t
    bias_row = jnp.concatenate([head_b[...]] * packed, axis=1)

    at = lax.broadcasted_iota(jnp.int32, (length, length), 0)
    to = lax.broadcasted_iota(jnp.int32, (length, length), 1)
    fold = length // packed
    order = ((at % fold) // quads) * count + (at // fold) * quads + at % quads
    shuffle[...] = jnp.where(order == to, 1.0, 0.0).astype(BF16)

    def multiply(kind):
        def outer_copy(dest, ch):
            return remote(
                prod.at[dest, :, places(kind, ch)], outer.at[:, channels(kind, place, ch)],
                sent_sem.at[0], o_recv.at[ch], block * per + dest,
            )

        for ch in range(chunks):
            now = places(kind, ch)
            drain(left_in.at[:, :, now], l_recv.at[ch])
            drain(right_in.at[pl.ds(0, groups - kind * plane), :, now], r_recv.at[0, ch])
            for h in range(cols_n):
                for c in range(edges[kind][ch], edges[kind][ch + 1]):
                    lhs = left_in[:, h, c].reshape(per * count, length)
                    rhs = right_in[:, h, c].reshape(length, length)
                    prod[:, h, c] = dot(lhs, rhs, NT).astype(BF16).reshape(per, count, length)
            each(per - 1, lambda d: outer_copy(lax.rem(slot + 1 + d, per), ch).start())
            pltpu.make_async_copy(
                prod.at[slot, :, now], outer.at[:, channels(kind, place, ch)], o_recv.at[ch]
            ).start()

    by_kind(multiply)

    def pieces(ch):
        for kind in range(2):
            for at in range(plane):
                start = kind * plane * sizes[0] + at * sizes[kind] + edges[kind][ch]
                yield start, start + span_of(kind, ch)

    stats = [None] * spans
    for ch in range(chunks):
        drain(outer.at[:, pl.ds(0, whole(ch))], o_recv.at[ch])
        if not whole(ch):
            continue
        for b in range(spans):
            amount = cols_n * whole(ch)
            span = slice(b * lanes, (b + 1) * lanes)
            loaded, added = [], 0.0
            for h in range(cols_n):
                for start, stop in pieces(ch):
                    values = outer[h, start:stop, :, span].astype(F32)
                    rows = slice((h * half + start) * count, (h * half + stop) * count)
                    outer_f[b, rows, :] = values.reshape((stop - start) * count, lanes)
                    added = added + jnp.sum(values, axis=0)
                    loaded.append((h, start, stop))
            middle, scatter = added * (1.0 / amount), 0.0
            for h, start, stop in loaded:
                rows = slice((h * half + start) * count, (h * half + stop) * count)
                centred = outer_f[b, rows, :].reshape(stop - start, count, lanes) - middle[None]
                scatter = scatter + jnp.sum(centred * centred, axis=0)
            if stats[b] is not None:
                before, mean_b, scatter_b = stats[b]
                apart = middle - mean_b
                scatter = scatter_b + scatter + apart * apart * (before * amount / (before + amount))
                middle = mean_b + apart * (amount / (before + amount))
                amount = before + amount
            stats[b] = (amount, middle, scatter)

    gain_col, shift_col = small[:, 5:6], small[:, 6:7]
    for b in range(spans):
        span = slice(b * lanes, (b + 1) * lanes)
        average = stats[b][1]
        inverse = lax.rsqrt(stats[b][2] * (1.0 / width) + 1.0)
        for i in range(count):
            part_i = outer_f[b, pl.ds(i, width, stride=count), :]
            part_i = (part_i - average[i:i + 1, :]) * inverse[i:i + 1, :] * gain_col + shift_col
            mixed = dot(part_i.astype(BF16), wo[...], TN) + b_out[...]
            rounded = (gate[i, span, :] * mixed).astype(BF16)
            update[i, span, :] = rounded
            new_pair[i, span, :] = (pair[i, span, :].astype(F32) + rounded.astype(F32)).astype(BF16)
    for i in range(quads):
        total = bias_row
        for p in range(packed):
            total = total + dot(new_pair[p * quads + i], spread_w[p], NT)
        logit_b[:, i] = total.astype(BF16).reshape(groups, count, 128)

    def logit_copy(dest):
        return remote(
            logit_b.at[dest], logit_in.at[me],
            sent_sem.at[0], m_recv.at[layer], dest,
        )

    logit_local = pltpu.make_async_copy(
        logit_b.at[me], logit_in.at[me], m_recv.at[layer]
    )
    each(groups - 1, lambda d: logit_copy(lax.rem(me + 1 + d, groups)).start())
    logit_local.start()

    bias_col = jnp.concatenate([head_b[...], jnp.zeros((7, bins), F32)], axis=0).T[:, 0:1]
    for i in range(count):
        own_t[i] = dot(head_t, new_pair[i], NT) + bias_col
    def sent(kind):
        for _ in range(1, cols_n):
            drain(wt.at[:, mine, :], sent_sem.at[0])
            drain(wo.at[mine, :], sent_sem.at[0])
        for ch in range(chunks):
            drain(left_b.at[:, pl.ds(0, whole(ch) - span_of(kind, ch))], sent_sem.at[0])
            drain(right_b.at[:, pl.ds(0, whole(ch) - span_of(kind, ch))], sent_sem.at[0])
            drain(right_b.at[:, pl.ds(0, plane * span_of(0, ch))], sent_sem.at[0])
            if kind:
                for _ in range(2):
                    drain(right_b.at[:, pl.ds(0, plane * span_of(1, ch))], sent_sem.at[0])
            drain(prod.at[pl.ds(0, per - 1), :, places(kind, ch)], sent_sem.at[0])

    by_kind(sent)

    tall = plane * quads * count
    for d in range(layers):
        at = lax.rem(layer + d, layers)
        some = logit_in.at[pl.ds(at * plane, plane)]
        drain(some, m_recv.at[at])
        logit_f[pl.ds(pl.multiple_of(at * tall, tall), tall), :] = some[...].astype(F32).reshape(tall, packed * bins)
    bin_id = lax.broadcasted_iota(jnp.int32, (bins, length), 0)
    for i in range(count):
        flipped = logit_f[pl.ds(i, groups * quads, stride=count), :].T
        flipped = jnp.concatenate([flipped[p * bins:(p + 1) * bins] for p in range(packed)], axis=1)
        symmetric = own_t[i] + dot(flipped.astype(BF16), shuffle[...])
        top = jnp.max(symmetric, axis=0, keepdims=True)
        total = top + jnp.log(jnp.sum(jnp.exp(symmetric - top), axis=0, keepdims=True))
        chosen = jnp.sum(jnp.where(bin_id == targets[i:i + 1, :], symmetric, 0.0), axis=0, keepdims=True)
        loss[i:i + 1, :] = pair_mask[i:i + 1, :] * (total - chosen)

    drain(logit_in.at[pl.ds(0, groups - 1)], sent_sem.at[0])


def finish(update, loss, update_out, loss_out, sem):
    first = pltpu.make_async_copy(update, update_out, sem.at[0])
    second = pltpu.make_async_copy(loss, loss_out, sem.at[1])
    first.start()
    second.start()
    first.wait()
    second.wait()


def local(rows_n, cols_n, *args):
    pair, residue_mask, targets, ln_gain, ln_shift, w_in, b_in, w_out, b_out, head_w, head_b = args
    count, length, width = pair.shape
    bins = head_w.shape[1]
    groups = rows_n * cols_n
    sup = SUPER
    per = groups // sup
    share = width // per
    chunks = 2
    part, half = share // cols_n, width // cols_n
    most = 2 * part - (part * FEW // 8 if part >= 4 else part)
    packed = 128 // bins
    quads = count // packed
    dma = pltpu.SemaphoreType.DMA
    vmem = pl.BlockSpec(memory_space=pltpu.VMEM)
    inputs = (
        pair, residue_mask.reshape(1, length), targets, ln_gain, ln_shift,
        jnp.swapaxes(w_in, 1, 2), b_in, w_out, b_out.reshape(1, width), head_w.T,
        head_b.reshape(1, bins),
    )
    update, loss = pl.pallas_call(
        functools.partial(kernel, rows_n, cols_n, sup, chunks),
        out_shape=(
            pltpu.VMEM(pair.shape, BF16),
            pltpu.VMEM((count, length), F32),
        ),
        in_specs=[pl.BlockSpec(memory_space=pl.ANY)] * 11,
        out_specs=(vmem, vmem),
        scratch_shapes=[pltpu.VMEM(x.shape, x.dtype) for x in inputs] + [
            pltpu.VMEM((5, width, width), BF16),
            pltpu.VMEM((width, width), BF16),
            pltpu.VMEM((width, 8), F32),
            pltpu.VMEM((count, length, width), BF16),
            pltpu.VMEM((length // 128, width // cols_n * count, 128), F32),
            pltpu.VMEM((cols_n, half, count, length), BF16),
            pltpu.VMEM((cols_n, half, count, length), BF16),
            pltpu.VMEM((per, cols_n, most, count, length), BF16),
            pltpu.VMEM((groups, cols_n, most, count, length), BF16),
            pltpu.VMEM((per, cols_n, most, count, length), BF16),
            pltpu.VMEM((cols_n, half, count, length), BF16),
            pltpu.VMEM((length // 128, width * count, 128), F32),
            pltpu.VMEM((count, length, width), F32),
            pltpu.VMEM((count, length, width), BF16),
            pltpu.VMEM((groups, quads, count, 128), BF16),
            pltpu.VMEM((groups, quads, count, 128), BF16),
            pltpu.VMEM((groups * quads * count, 128), F32),
            pltpu.VMEM((count, bins, length), F32),
            dma((1,)), dma((2,)), dma((chunks,)), dma((2, chunks)), dma((chunks,)),
            dma((groups // (per // 2),)),
            dma((1,)), pltpu.SemaphoreType.REGULAR,
            pltpu.VMEM((packed, 128, width), BF16), pltpu.VMEM((length, length), BF16),
        ],
        compiler_params=pltpu.CompilerParams(
            collective_id=0, has_side_effects=True, vmem_limit_bytes=60 * 1024 * 1024
        ),
    )(*inputs)
    anywhere = pl.BlockSpec(memory_space=pl.ANY)
    return pl.pallas_call(
        finish,
        out_shape=(
            jax.ShapeDtypeStruct(update.shape, update.dtype), jax.ShapeDtypeStruct(loss.shape, loss.dtype),
        ),
        in_specs=[pl.BlockSpec(memory_space=pltpu.VMEM)] * 2, compiler_params=pltpu.CompilerParams(vmem_limit_bytes=1024*1024),
        out_specs=(anywhere, anywhere),
        scratch_shapes=[dma((2,))],
    )(update, loss)


def solution(mesh):
    placed = (
        P(("ga", "row", "col"), None, None),
        P("ga"),
        P(("ga", "row", "col"), None),
        P(),
        P(),
        P(None, None, "col"),
        P(),
        P("col", None),
        P(),
        P(),
        P(),
    )
    return jax.shard_map(
        functools.partial(local, mesh.shape["row"], mesh.shape["col"]),
        mesh=mesh,
        in_specs=placed,
        out_specs=(P(("ga", "row", "col"), None, None), P(("ga", "row", "col"), None)),
        check_vma=False,
    )
```

```python
import functools

import jax
import jax.numpy as jnp
from jax import lax
from jax.experimental import pallas as pl
from jax.experimental.pallas import tpu as pltpu
from jax.sharding import PartitionSpec as P

SUPER = 2
FEW = 7
CUT = 6
F32, BF16 = jnp.float32, jnp.bfloat16
NT = (((1,), (1,)), ((), ()))
TN = (((0,), (0,)), ((), ()))


def dot(lhs, rhs, dims=(((1,), (0,)), ((), ()))):
    return lax.dot_general(lhs, rhs, dims, preferred_element_type=F32)


def kernel(
    rows_n, cols_n, sup, chunks,
    *refs,
):
    sources, (update, loss) = refs[:11], refs[11:13]
    held, rest = refs[13:24], refs[24:]
    (pair, mask, targets, ln_gain, ln_shift, w_in, b_in, w_out, b_out, head_w, head_b) = held
    (
    wt, wo, small, normed, side_f, right_b, left_b, left_in, right_in, prod, outer, outer_f, gate,
        new_pair, logit_b, logit_in, logit_f, own_t,
        sent_sem, w_recv, l_recv, r_recv, o_recv, m_recv,
        in_sem, far_sem, spread_w, shuffle,
    ) = rest
    groups = rows_n * cols_n
    count, length, width = pair.shape
    bins = head_w.shape[0]
    per = groups // sup
    share = width // per
    part = share // cols_n
    few = part * FEW // 8 if part >= 4 else part
    sizes = (few, 2 * part - few)
    edges = [[0, max(size * CUT // 8, 1), size] for size in sizes]
    half = w_in.shape[1]
    lanes = 128
    spans = length // lanes
    packed = 128 // bins
    quads = count // packed
    col = lax.axis_index("col")
    me = lax.axis_index("row") * cols_n + col
    block, slot = lax.div(me, per), lax.rem(me, per)
    plane = per // 2
    layer, place = lax.div(me, plane), lax.rem(me, plane)
    inner = lax.rem(layer + block, 2) == 1
    layers = groups // plane

    def where(peer):
        return {"row": lax.div(peer, cols_n), "col": lax.rem(peer, cols_n)}

    def remote(src, dst, send, recv, peer):
        return pltpu.make_async_remote_copy(
            src_ref=src, dst_ref=dst, send_sem=send, recv_sem=recv,
            device_id=where(peer), device_id_type=pl.DeviceIdType.MESH,
        )

    def each(n, body):
        lax.fori_loop(0, n, lambda i, c: (body(i), c)[1], 0, unroll=True)

    loads = [pltpu.make_async_copy(sources[n], held[n], in_sem.at[int(n not in (0, 3, 4))]) for n in range(11)]
    for load in loads:
        load.start()
    barrier = pltpu.get_barrier_semaphore()

    def greet(d):
        peer = lax.rem(me + 1 + d, groups)
        apart = lax.div(peer, plane) - layer

        @pl.when(apart * apart < 2)
        def _():
            pl.semaphore_signal(
                barrier, inc=1, device_id=where(peer), device_id_type=pl.DeviceIdType.MESH
            )

    each(groups - 1, greet)

    def drain(ref, sem):
        pltpu.make_async_copy(ref, ref, sem).wait()


    for n in (0, 3, 4):
        loads[n].wait()
    mine = pl.ds(pl.multiple_of(col * half, half), half)

    def norm_rows(i):
        values = pair[i].astype(F32)
        centred = values - jnp.mean(values, axis=-1, keepdims=True)
        spread = jnp.mean(centred * centred, axis=-1, keepdims=True)
        scaled = centred * lax.rsqrt(spread + 0.1) * ln_gain[0:1, :] + ln_shift[0:1, :]
        normed[i] = scaled.astype(BF16)

    each(count, norm_rows)
    for n in (1, 2, 5, 6, 7, 8, 9, 10):
        loads[n].wait()
    wt[:, mine, :] = w_in[...]
    wo[mine, :] = w_out[...]

    row_mask = mask[...].astype(F32)
    lane = lax.broadcasted_iota(jnp.int32, (count, length), 1)
    sub = lax.broadcasted_iota(jnp.int32, (count, length), 0)
    own_mask = jnp.sum(jnp.where(lane == me * count + sub, row_mask, 0.0), axis=1, keepdims=True)
    pair_mask = own_mask * row_mask

    small[...] = jnp.concatenate(
        [b_in[...], ln_gain[1:2, :], ln_shift[1:2, :], jnp.zeros((1, width), F32)], axis=0
    ).T

    def weight_copies(peer_col):
        peer = me - col + peer_col
        return (
            remote(wt.at[:, mine, :], wt.at[:, mine, :], sent_sem.at[0], w_recv.at[0], peer),
            remote(wo.at[mine, :], wo.at[mine, :], sent_sem.at[0], w_recv.at[1], peer),
        )

    def wait_weights(which):
        for d in range(1, cols_n):
            peer_col = lax.rem(col + d, cols_n)
            theirs = pl.ds(pl.multiple_of(peer_col * half, half), half)
            ref = (wt.at[:, theirs, :], wo.at[theirs, :])[which]
            drain(ref, w_recv.at[which])

    def make_side(first, out, span_w):
        start = pl.multiple_of(span_w * half, half)
        rows = pl.ds(start, half)
        weights = wt[first:first + 2, rows, :].reshape(2 * half, width)
        value_b, gate_b = small[rows, first:first + 1], small[rows, first + 1:first + 2]

        for i in range(count):
            both = dot(weights, normed[i], NT)
            value = jax.nn.sigmoid(both[half:] + gate_b) * (both[:half] + value_b)
            for b in range(spans):
                side_f[b, pl.ds(i, half, stride=count), :] = value[:, b * lanes:(b + 1) * lanes]
        for b in range(spans):
            span = slice(b * lanes, (b + 1) * lanes)
            masked = side_f[b].reshape(half, count, lanes) * pair_mask[:, span][None]
            out[span_w, :, :, span] = masked.astype(BF16)

    def span_of(kind, ch):
        return edges[kind][ch + 1] - edges[kind][ch]

    def whole(ch):
        return plane * (span_of(0, ch) + span_of(1, ch))

    def channels(kind, at, ch):
        return pl.ds(kind * plane * sizes[0] + at * sizes[kind] + edges[kind][ch], span_of(kind, ch))

    def places(kind, ch):
        return pl.ds(edges[kind][ch], span_of(kind, ch))

    def device(kind, part_of, at):
        return part_of * per + lax.rem(kind + part_of, 2) * plane + at

    def by_kind(body):
        pl.when(inner)(functools.partial(body, 1))
        pl.when(jnp.logical_not(inner))(functools.partial(body, 0))

    def left_copy(kind, at, ch, h):
        return remote(
            left_b.at[h, channels(kind, at, ch)], left_in.at[slot, h, places(kind, ch)],
            sent_sem.at[0], l_recv.at[ch], device(kind, block, at),
        )

    def right_copy(kind, part_of, at, ch, h, way=0):
        return remote(
            right_b.at[h, channels(kind, at, ch)], right_in.at[me, h, places(kind, ch)],
            sent_sem.at[0], r_recv.at[way, ch], device(kind, part_of, at),
        )

    def pass_on(ch):
        def one(d):
            piece = right_in.at[3 * block * plane + lax.rem(place + d, plane), :, places(1, ch)]
            remote(
                piece, piece, sent_sem.at[0], r_recv.at[0, ch], device(1, 1 - block, place)
            ).start()

        each(plane, one)

    def send_right(kind, ch, h):
        way = kind * (1 - inner.astype(jnp.int32))

        def one(d):
            at = lax.rem(place + d, plane)

            @pl.when(device(kind, block, at) != me)
            def _():
                right_copy(kind, block, at, ch, h, way).start()

        each(plane, one)

    def send_left(kind, ch, h):
        def one(d):
            at = lax.rem(place + d, plane)

            @pl.when(device(kind, block, at) != me)
            def _():
                left_copy(kind, at, ch, h).start()

        each(plane, one)

    def send_block(ch, h):
        for kind in (1, 0):
            send_right(kind, ch, h)
            send_left(kind, ch, h)

    def send_across(kind, ch, h):
        def one(d):
            right_copy(kind, 1 - block, lax.rem(place + d, plane), ch, h).start()

        each(plane, one)

    def keep(ch):
        def own(kind):
            pltpu.make_async_copy(
                right_b.at[:, channels(kind, place, ch)], right_in.at[me, :, places(kind, ch)], r_recv.at[0, ch]
            ).start()
            pltpu.make_async_copy(
                left_b.at[:, channels(kind, place, ch)], left_in.at[slot, :, places(kind, ch)], l_recv.at[ch]
            ).start()

        by_kind(own)

    make_side(2, right_b, col)
    pl.semaphore_wait(barrier, plane * (2 + inner.astype(jnp.int32)) - 1)

    def tell(peer):
        pl.semaphore_signal(far_sem, inc=1, device_id=where(peer), device_id_type=pl.DeviceIdType.MESH)

    @pl.when(inner)
    def _():
        tell(me + plane - 2 * plane * block)

    for d in range(1, cols_n):
        for copy in weight_copies(lax.rem(col + d, cols_n)):
            copy.start()
    for turn in range(cols_n):
        h = lax.rem(col + turn, cols_n)
        if turn:
            if turn == 1:
                wait_weights(0)
            make_side(2, right_b, h)
        pl.when(inner)(functools.partial(send_across, 1, 0, h))
        pl.when(jnp.logical_not(inner))(functools.partial(send_right, 1, 0, h))
        make_side(0, left_b, h)
        send_left(1, 0, h)
        pl.when(inner)(functools.partial(send_right, 1, 0, h))
        send_left(0, 0, h)
        send_right(0, 0, h)
    keep(0)
    every = slice(None)

    @pl.when(jnp.logical_not(inner))
    def _():
        send_right(1, 1, every)

    pl.semaphore_wait(far_sem, 1)

    @pl.when(inner)
    def _():
        tell(me - plane + 2 * plane * block)
        send_across(0, 0, every)
        send_across(0, 1, every)
        send_block(1, every)

    @pl.when(jnp.logical_not(inner))
    def _():
        send_across(0, 0, every)
        send_left(1, 1, every)
        send_left(0, 1, every)
        send_right(0, 1, every)
        send_across(0, 1, every)

    keep(1)

    def make_gate(i):
        gate[i] = jax.nn.sigmoid(dot(normed[i], wt[4], NT) + b_in[4:5, :])

    each(count, make_gate)

    @pl.when(inner)
    def _():
        for ch in range(chunks):
            drain(right_in.at[pl.ds(0, plane), :, places(1, ch)], r_recv.at[1, ch])
            pass_on(ch)
            if ch == 0:
                send_across(1, 1, every)

    wait_weights(1)

    head_t = head_w[...]
    spread_w[...] = jnp.zeros(spread_w.shape, BF16)
    for p in range(packed):
        spread_w[p, p * bins:(p + 1) * bins, :] = head_t
    bias_row = jnp.concatenate([head_b[...]] * packed, axis=1)

    at = lax.broadcasted_iota(jnp.int32, (length, length), 0)
    to = lax.broadcasted_iota(jnp.int32, (length, length), 1)
    fold = length // packed
    order = ((at % fold) // quads) * count + (at // fold) * quads + at % quads
    shuffle[...] = jnp.where(order == to, 1.0, 0.0).astype(BF16)

    def multiply(kind):
        def outer_copy(dest, ch):
            return remote(
                prod.at[dest, :, places(kind, ch)], outer.at[:, channels(kind, place, ch)],
                sent_sem.at[0], o_recv.at[ch], block * per + dest,
            )

        for ch in range(chunks):
            now = places(kind, ch)
            drain(left_in.at[:, :, now], l_recv.at[ch])
            drain(right_in.at[pl.ds(0, groups - kind * plane), :, now], r_recv.at[0, ch])
            for h in range(cols_n):
                for c in range(edges[kind][ch], edges[kind][ch + 1]):
                    lhs = left_in[:, h, c].reshape(per * count, length)
                    rhs = right_in[:, h, c].reshape(length, length)
                    prod[:, h, c] = dot(lhs, rhs, NT).astype(BF16).reshape(per, count, length)
            each(per - 1, lambda d: outer_copy(lax.rem(slot + 1 + d, per), ch).start())
            pltpu.make_async_copy(
                prod.at[slot, :, now], outer.at[:, channels(kind, place, ch)], o_recv.at[ch]
            ).start()

    by_kind(multiply)

    def pieces(ch):
        for kind in range(2):
            for at in range(plane):
                start = kind * plane * sizes[0] + at * sizes[kind] + edges[kind][ch]
                yield start, start + span_of(kind, ch)

    stats = [None] * spans
    for ch in range(chunks):
        drain(outer.at[:, pl.ds(0, whole(ch))], o_recv.at[ch])
        if not whole(ch):
            continue
        for b in range(spans):
            amount = cols_n * whole(ch)
            span = slice(b * lanes, (b + 1) * lanes)
            loaded, added = [], 0.0
            for h in range(cols_n):
                for start, stop in pieces(ch):
                    values = outer[h, start:stop, :, span].astype(F32)
                    rows = slice((h * half + start) * count, (h * half + stop) * count)
                    outer_f[b, rows, :] = values.reshape((stop - start) * count, lanes)
                    added = added + jnp.sum(values, axis=0)
                    loaded.append((h, start, stop))
            middle, scatter = added * (1.0 / amount), 0.0
            for h, start, stop in loaded:
                rows = slice((h * half + start) * count, (h * half + stop) * count)
                centred = outer_f[b, rows, :].reshape(stop - start, count, lanes) - middle[None]
                scatter = scatter + jnp.sum(centred * centred, axis=0)
            if stats[b] is not None:
                before, mean_b, scatter_b = stats[b]
                apart = middle - mean_b
                scatter = scatter_b + scatter + apart * apart * (before * amount / (before + amount))
                middle = mean_b + apart * (amount / (before + amount))
                amount = before + amount
            stats[b] = (amount, middle, scatter)

    gain_col, shift_col = small[:, 5:6], small[:, 6:7]
    for b in range(spans):
        span = slice(b * lanes, (b + 1) * lanes)
        average = stats[b][1]
        inverse = lax.rsqrt(stats[b][2] * (1.0 / width) + 1.0)
        for i in range(count):
            part_i = outer_f[b, pl.ds(i, width, stride=count), :]
            part_i = (part_i - average[i:i + 1, :]) * inverse[i:i + 1, :] * gain_col + shift_col
            mixed = dot(part_i.astype(BF16), wo[...], TN) + b_out[...]
            rounded = (gate[i, span, :] * mixed).astype(BF16)
            update[i, span, :] = rounded
            new_pair[i, span, :] = (pair[i, span, :].astype(F32) + rounded.astype(F32)).astype(BF16)
    for i in range(quads):
        total = bias_row
        for p in range(packed):
            total = total + dot(new_pair[p * quads + i], spread_w[p], NT)
        logit_b[:, i] = total.astype(BF16).reshape(groups, count, 128)

    def logit_copy(dest):
        return remote(
            logit_b.at[dest], logit_in.at[me],
            sent_sem.at[0], m_recv.at[layer], dest,
        )

    logit_local = pltpu.make_async_copy(
        logit_b.at[me], logit_in.at[me], m_recv.at[layer]
    )
    each(groups - 1, lambda d: logit_copy(lax.rem(me + 1 + d, groups)).start())
    logit_local.start()

    bias_col = jnp.concatenate([head_b[...], jnp.zeros((7, bins), F32)], axis=0).T[:, 0:1]
    for i in range(count):
        own_t[i] = dot(head_t, new_pair[i], NT) + bias_col
    def sent(kind):
        for _ in range(1, cols_n):
            drain(wt.at[:, mine, :], sent_sem.at[0])
            drain(wo.at[mine, :], sent_sem.at[0])
        for ch in range(chunks):
            drain(left_b.at[:, pl.ds(0, whole(ch) - span_of(kind, ch))], sent_sem.at[0])
            drain(right_b.at[:, pl.ds(0, whole(ch) - span_of(kind, ch))], sent_sem.at[0])
            drain(right_b.at[:, pl.ds(0, plane * span_of(0, ch))], sent_sem.at[0])
            if kind:
                for _ in range(2):
                    drain(right_b.at[:, pl.ds(0, plane * span_of(1, ch))], sent_sem.at[0])
            drain(prod.at[pl.ds(0, per - 1), :, places(kind, ch)], sent_sem.at[0])

    by_kind(sent)

    tall = plane * quads * count
    for d in range(layers):
        at = lax.rem(layer + d, layers)
        some = logit_in.at[pl.ds(at * plane, plane)]
        drain(some, m_recv.at[at])
        logit_f[pl.ds(pl.multiple_of(at * tall, tall), tall), :] = some[...].astype(F32).reshape(tall, packed * bins)
    bin_id = lax.broadcasted_iota(jnp.int32, (bins, length), 0)
    for i in range(count):
        flipped = logit_f[pl.ds(i, groups * quads, stride=count), :].T
        flipped = jnp.concatenate([flipped[p * bins:(p + 1) * bins] for p in range(packed)], axis=1)
        symmetric = own_t[i] + dot(flipped.astype(BF16), shuffle[...])
        top = jnp.max(symmetric, axis=0, keepdims=True)
        total = top + jnp.log(jnp.sum(jnp.exp(symmetric - top), axis=0, keepdims=True))
        chosen = jnp.sum(jnp.where(bin_id == targets[i:i + 1, :], symmetric, 0.0), axis=0, keepdims=True)
        loss[i:i + 1, :] = pair_mask[i:i + 1, :] * (total - chosen)

    drain(logit_in.at[pl.ds(0, groups - 1)], sent_sem.at[0])


def finish(update, loss, update_out, loss_out, sem):
    first = pltpu.make_async_copy(update, update_out, sem.at[0])
    second = pltpu.make_async_copy(loss, loss_out, sem.at[1])
    first.start()
    second.start()
    first.wait()
    second.wait()


def local(rows_n, cols_n, *args):
    pair, residue_mask, targets, ln_gain, ln_shift, w_in, b_in, w_out, b_out, head_w, head_b = args
    count, length, width = pair.shape
    bins = head_w.shape[1]
    groups = rows_n * cols_n
    sup = SUPER
    per = groups // sup
    share = width // per
    chunks = 2
    part, half = share // cols_n, width // cols_n
    most = 2 * part - (part * FEW // 8 if part >= 4 else part)
    packed = 128 // bins
    quads = count // packed
    dma = pltpu.SemaphoreType.DMA
    vmem = pl.BlockSpec(memory_space=pltpu.VMEM)
    inputs = (
        pair, residue_mask.reshape(1, length), targets, ln_gain, ln_shift,
        jnp.swapaxes(w_in, 1, 2), b_in, w_out, b_out.reshape(1, width), head_w.T,
        head_b.reshape(1, bins),
    )
    update, loss = pl.pallas_call(
        functools.partial(kernel, rows_n, cols_n, sup, chunks),
        out_shape=(
            pltpu.VMEM(pair.shape, BF16),
            pltpu.VMEM((count, length), F32),
        ),
        in_specs=[pl.BlockSpec(memory_space=pl.ANY)] * 11,
        out_specs=(vmem, vmem),
        scratch_shapes=[pltpu.VMEM(x.shape, x.dtype) for x in inputs] + [
            pltpu.VMEM((5, width, width), BF16),
            pltpu.VMEM((width, width), BF16),
            pltpu.VMEM((width, 8), F32),
            pltpu.VMEM((count, length, width), BF16),
            pltpu.VMEM((length // 128, width // cols_n * count, 128), F32),
            pltpu.VMEM((cols_n, half, count, length), BF16),
            pltpu.VMEM((cols_n, half, count, length), BF16),
            pltpu.VMEM((per, cols_n, most, count, length), BF16),
            pltpu.VMEM((groups, cols_n, most, count, length), BF16),
            pltpu.VMEM((per, cols_n, most, count, length), BF16),
            pltpu.VMEM((cols_n, half, count, length), BF16),
            pltpu.VMEM((length // 128, width * count, 128), F32),
            pltpu.VMEM((count, length, width), F32),
            pltpu.VMEM((count, length, width), BF16),
            pltpu.VMEM((groups, quads, count, 128), BF16),
            pltpu.VMEM((groups, quads, count, 128), BF16),
            pltpu.VMEM((groups * quads * count, 128), F32),
            pltpu.VMEM((count, bins, length), F32),
            dma((1,)), dma((2,)), dma((chunks,)), dma((2, chunks)), dma((chunks,)),
            dma((groups // (per // 2),)),
            dma((2,)), pltpu.SemaphoreType.REGULAR,
            pltpu.VMEM((packed, 128, width), BF16), pltpu.VMEM((length, length), BF16),
        ],
        compiler_params=pltpu.CompilerParams(
            collective_id=0, has_side_effects=True, vmem_limit_bytes=60 * 1024 * 1024
        ),
    )(*inputs)
    anywhere = pl.BlockSpec(memory_space=pl.ANY)
    return pl.pallas_call(
        finish,
        out_shape=(
            jax.ShapeDtypeStruct(update.shape, update.dtype), jax.ShapeDtypeStruct(loss.shape, loss.dtype),
        ),
        in_specs=[pl.BlockSpec(memory_space=pltpu.VMEM)] * 2, compiler_params=pltpu.CompilerParams(vmem_limit_bytes=1024*1024),
        out_specs=(anywhere, anywhere),
        scratch_shapes=[dma((2,))],
    )(update, loss)


def solution(mesh):
    placed = (
        P(("ga", "row", "col"), None, None),
        P("ga"),
        P(("ga", "row", "col"), None),
        P(),
        P(),
        P(None, None, "col"),
        P(),
        P("col", None),
        P(),
        P(),
        P(),
    )
    return jax.shard_map(
        functools.partial(local, mesh.shape["row"], mesh.shape["col"]),
        mesh=mesh,
        in_specs=placed,
        out_specs=(P(("ga", "row", "col"), None, None), P(("ga", "row", "col"), None)),
        check_vma=False,
    )
```
